32 devices in a mesh: section: 4 (over y, x), owner: 8 (over z, core).
Axes of the slice: x: 2, y: 2, z: 4, core: 2. Of those that a mesh axis runs over, the one named last changes fastest.
Arguments:
- probe_values: bfloat16 [8, 8192, 128], P('section', 'owner'), may hold values from -6 to 6
- probe_keys: int32 [8, 8192], P('section', 'owner'), may hold values from 0 to 2047
- group_ids: int32 [8, 8192], P('section', 'owner'), may hold values from 0 to 127
- block_dest: int32 [8, 64, 1], P('section', 'owner'), may hold values from 0 to 7; in each aligned block of 8 rows (0 to 7, 8 to 15, ..., all dimensions but the last counted through in order) at most 2 rows name the same one
- filter_bits: int32 [4, 8, 512], P('section', None, 'owner'), may hold values from 0 to 65535, as said below
- section_weights: bfloat16 [4, 128, 128], P('section'), may hold values from -0.5 to 0.5
- build_keys: int32 [32768], P('owner'), may hold values from 0 to 2047
- build_values: bfloat16 [32768, 128], P('owner'), may hold values from -6 to 6
Outputs:
- group_sums: float32 [128, 128], P(('section', 'owner'))
The draws below stay inside these ranges and needn't reach their ends.
Inputs may be any that keep to these rules, and one draw needn't show every extreme that they name: `block_dest`: in each micro-batch, no owner is named by more than 2 of the 8 blocks of one device, a bound that some block reaches. `filter_bits`: bit b of a word is the keep bit of row 16 w + b; the upper bits are 0.
All inputs are finite; a program needn't handle non-finite values.
Results may differ from the reference program's by a relative error of at most 0.012.
Values may be sent and summed in bfloat16 or wider, within the bound.
No kernel may reach another device: no remote copies, remote signals or barrier semaphores. Data moves between devices by JAX's collectives and lax.ppermute only.
A program may use at most 128 MiB of HBM per device.

```python
import math
import jax
import jax.numpy as jnp
import numpy as np

P_SIZE = 128
BLOCK = 128
CAP = 2
MBS = 2
KEYS_OWN = 2048
BUILD_OWN = 4096
MB = 8
NB = 8
ROWS = 8192
WORDS = 512
BUILD = 32768
GROUPS = 128
N_SECTION = 4
N_OWNER = 8


def draw_filter_bits(key, part):
    lower_bits = jax.random.randint(jax.random.fold_in(key, 11), (N_SECTION, MB, WORDS), 0, 65536, dtype=jnp.int32)
    upper_bits = jax.random.randint(jax.random.fold_in(key, 12), (N_SECTION, MB, WORDS), 0, 65536, dtype=jnp.int32)
    return lower_bits | upper_bits


def set_ends(result, own_key, smallest, largest):
    index_at = [jax.random.randint(jax.random.fold_in(own_key, axis), (), 0, length) for axis, length in enumerate(result.shape)]
    main_axis = result.shape.index(max(result.shape))
    next_to = index_at[:main_axis] + [(index_at[main_axis] + 1) % result.shape[main_axis]] + index_at[main_axis + 1:]
    return result.at[tuple(index_at)].set(smallest).at[tuple(next_to)].set(largest)


def levels(key, extent, pieces, smallest, high):
    def one(position, shards_of):
        heights = jax.random.uniform(jax.random.fold_in(jax.random.fold_in(key, 6), position), (shards_of,), jnp.float32, smallest / len(pieces), high / len(pieces))
        return jnp.repeat(jnp.exp(heights), extent[position] // shards_of).reshape((-1,) + (1,) * (len(extent) - position - 1))

    gain = one(*pieces[0])
    for cut in pieces[1:]:
        gain = gain * one(*cut)
    return gain


def deal_out(rng, own, number, rows, amount, top, bound, lean):
    sequence = jax.random.permutation(rng, amount)
    heavy_load, ordinary = portions_of(amount, rows * top, bound, lean, True), portions_of(amount, rows * top, bound, lean, False)
    places = jnp.arange(amount)

    def named(sizes, offset_by):
        used = int((sizes > 0).sum())
        fixed = max(1, used // 4)
        passed = fixed + (places - fixed + offset_by * (used - fixed)) % max(1, amount - fixed)
        return jnp.zeros((amount,), jnp.int32).at[sequence[jnp.where(places < fixed, places, passed)]].set(jnp.asarray(sizes, jnp.int32))

    sizes = jnp.where(number % 4 == 0, named(heavy_load, number // 4), named(ordinary, number - number // 4 - 1))
    mixed = jax.random.permutation(jax.random.fold_in(own, 3), amount)
    donor, receiver = mixed[0:amount // 2 * 2:2], mixed[1:amount // 2 * 2:2]
    room = jnp.minimum(sizes[donor] - 1, bound - sizes[receiver]) // 2
    room = jnp.where((donor == sequence[0]) | (receiver == sequence[0]) | (sizes[receiver] == 0), 0, jnp.maximum(room, 0))
    passed = jax.random.randint(jax.random.fold_in(own, 4), (amount // 2,), 0, 1 << 20) % (room + 1)
    sizes = sizes.at[donor].add(-passed).at[receiver].add(passed)
    items = jnp.searchsorted(jnp.cumsum(sizes), jnp.arange(rows * top), side="right").astype(jnp.int32)
    grid = items.reshape(top, rows).T
    grid = grid[jax.random.permutation(jax.random.fold_in(own, 1), rows)]
    offset_by = jax.random.randint(jax.random.fold_in(own, 2), (rows, 1), 0, top)
    return jnp.take_along_axis(grid, (jnp.arange(top)[None, :] + offset_by) % top, axis=1)


def portions_of(amount, total, most, lean, full):
    portions = [(1 << 20) // math.isqrt(standing ** lean) + 1 for standing in range(1, amount + 1)]
    largest = most if full else min(most, max(-(-total // amount), total * portions[0] // sum(portions)))
    least = 1 if total - largest >= amount - 1 else 0
    counts, spare = [largest] + [least] * (amount - 1), total - largest - least * (amount - 1)
    while spare > 0:
        candidates = [i for i in range(1, amount) if counts[i] < largest] or [i for i in range(1, amount) if counts[i] < most]
        mass, remaining = sum([portions[i] for i in candidates]), spare
        for i in candidates:
            extra = min(most - counts[i], max(1, remaining * portions[i] // mass), spare)
            counts[i] = counts[i] + extra
            spare = spare - extra
    return np.array(counts)


def centred(stream_key, extent, scale, most, shards=(), kind=jnp.bfloat16):
    entries = jax.random.normal(stream_key, extent, jnp.float32) * scale
    if len(shards) > 0:
        entries = levels(stream_key, extent, shards, -0.22, 0.18) * entries
    return jnp.clip(entries, min=-most, max=most).astype(kind)


def setup_inputs(seed: int = 0) -> dict:
    arg_keys = jax.random.split(jax.random.key(seed), 9)
    probe_values = centred(arg_keys[0], (MB, ROWS, P_SIZE), 1.0, 6.0, ((0, 4), (1, 8)))
    probe_keys = set_ends(jax.random.randint(arg_keys[1], (MB, ROWS), 0, KEYS_OWN), jax.random.fold_in(arg_keys[1], 1), 0, KEYS_OWN - 1).astype(jnp.int32)
    group_ids = set_ends(jax.random.randint(arg_keys[2], (MB, ROWS), 0, GROUPS), jax.random.fold_in(arg_keys[2], 1), 0, GROUPS - 1).astype(jnp.int32)
    block_dest_keys = jax.random.split(jax.random.fold_in(arg_keys[3], 1), MB * (NB * N_OWNER) // NB)
    block_dest_turns = jax.random.permutation(jax.random.fold_in(arg_keys[3], 3), MB * (NB * N_OWNER) // NB)
    block_dest = jax.vmap(lambda own, number: deal_out(jax.random.fold_in(arg_keys[3], 2), own, number, NB, N_OWNER, 1, CAP, 2))(block_dest_keys, block_dest_turns).reshape((MB, NB * N_OWNER, 1))
    filter_bits = draw_filter_bits(jax.random.fold_in(arg_keys[8], 71), 0)
    section_weights = centred(arg_keys[5], (N_SECTION, P_SIZE, P_SIZE), P_SIZE ** -0.5, 0.5, ((0, 4),))
    build_keys = set_ends(jax.random.randint(arg_keys[6], (BUILD,), 0, KEYS_OWN), jax.random.fold_in(arg_keys[6], 1), 0, KEYS_OWN - 1).astype(jnp.int32)
    build_values = centred(arg_keys[7], (BUILD, P_SIZE), 1.0, 6.0, ((0, 8),))
    return dict(probe_values=probe_values, probe_keys=probe_keys, group_ids=group_ids, block_dest=block_dest, filter_bits=filter_bits, section_weights=section_weights, build_keys=build_keys, build_values=build_values)


def unpack_bits(bit_words):
    shifts = jnp.arange(16, dtype=jnp.int32)
    spread = jnp.right_shift(bit_words[..., None], shifts) & 1
    return spread.reshape(bit_words.shape[:-1] + (bit_words.shape[-1] * 16,)).astype(jnp.float32)


def apply_section(payload, kept_mask, weight):
    columns = payload.shape[-1]
    projected = jnp.dot(payload.reshape(-1, columns), weight, preferred_element_type=jnp.float32)
    projected = projected.reshape(payload.shape)
    updated = kept_mask[..., None] * (payload.astype(jnp.float32) + jax.nn.silu(projected))
    return updated.astype(jnp.bfloat16)


def reference(probe_values, probe_keys, group_ids, block_dest, filter_bits, section_weights, build_keys, build_values):
    owners = (jnp.arange(N_OWNER * BUILD_OWN, dtype=jnp.int32) // BUILD_OWN).astype(jnp.int32)
    key_table = jax.ops.segment_sum(build_values.astype(jnp.float32), owners * KEYS_OWN + build_keys.astype(jnp.int32), num_segments=N_OWNER * KEYS_OWN)
    group_sums = jnp.zeros((GROUPS, P_SIZE), jnp.float32)
    for micro in range(MB):
        home_section = micro // MBS
        payload = probe_values[micro]
        for step_number in range(N_SECTION):
            section_at = (home_section + step_number) % N_SECTION
            kept_mask = unpack_bits(filter_bits[section_at, micro])
            payload = apply_section(payload, kept_mask, section_weights[section_at])
        dest_rows = jnp.repeat(block_dest[micro, :, 0], BLOCK).astype(jnp.int32)
        matched = jnp.take(key_table, dest_rows * KEYS_OWN + probe_keys[micro].astype(jnp.int32), axis=0)
        joined = (payload.astype(jnp.float32) * matched).astype(jnp.bfloat16)
        group_sums = group_sums + jax.ops.segment_sum(joined.astype(jnp.float32), group_ids[micro].astype(jnp.int32), num_segments=GROUPS)
    return group_sums
```

```python
import functools

import jax
import jax.numpy as jnp
from jax import lax
from jax.experimental import pallas as pl
from jax.experimental.pallas import tpu as pltpu
from jax.sharding import PartitionSpec as P

CAP = 2
KEYS_OWN = 2048
GRP_DEV = 4
META = 16
BF16 = jnp.bfloat16
F32 = jnp.float32


def vmem():
    return pl.BlockSpec(memory_space=pltpu.VMEM)


def smem():
    return pl.BlockSpec(memory_space=pltpu.SMEM)


def params():
    return pltpu.CompilerParams(vmem_limit_bytes=56 * 2**20)


def walk_blocks(dest_ref, count_ref, owners, batches, blocks, visit):
    def clear(owner, carry):
        count_ref[owner] = 0
        return carry

    lax.fori_loop(0, owners, clear, 0)
    for micro in range(batches):

        def step(block, carry, micro=micro):
            owner = dest_ref[micro, block]
            slot = count_ref[owner]
            count_ref[owner] = slot + 1
            visit(micro, block, owner, slot)
            return carry

        lax.fori_loop(0, blocks, step, 0, unroll=min(blocks, 8))


def pack_first(early, rows, dest_ref, values_ref, keys_ref, groups_ref, out_ref, meta_ref, count_ref):
    owners = out_ref.shape[0]
    batches, blocks = dest_ref.shape
    meta_ref[...] = jnp.zeros_like(meta_ref)
    out_ref[...] = jnp.zeros_like(out_ref)

    def visit(micro, block, owner, slot):
        lanes = pl.ds(pl.multiple_of(block * rows, rows), rows)

        @pl.when(slot < early)
        def _():
            out_ref[owner, pl.ds(pl.multiple_of(slot * rows, rows), rows), :] = values_ref[micro * blocks + block]
            keys = keys_ref[pl.ds(micro, 1), lanes]
            groups = groups_ref[pl.ds(micro, 1), lanes]
            base = slot * 4
            meta_ref[owner, pl.ds(base, 1), :] = (keys >> 7).astype(F32)
            meta_ref[owner, pl.ds(base + 1, 1), :] = (keys & 127).astype(F32)
            meta_ref[owner, pl.ds(base + 2, 1), :] = (groups >> 7).astype(F32)
            meta_ref[owner, pl.ds(base + 3, 1), :] = (groups & 127).astype(F32)

    walk_blocks(dest_ref, count_ref, owners, batches, blocks, visit)
    out_ref[:, early * rows :, :] = meta_ref[...].astype(BF16)


def pack_last(early, rows, dest_ref, values_ref, keys_ref, groups_ref, bits_ref, out_ref, meta_ref, kept_ref, count_ref):
    owners = out_ref.shape[0]
    batches, blocks = dest_ref.shape
    late_slots = (out_ref.shape[1] - META) // rows
    meta_ref[...] = jnp.zeros_like(meta_ref)
    out_ref[...] = jnp.zeros_like(out_ref)
    mask_base = late_slots * 4
    all_kept = bits_ref[0].astype(F32)
    for section in range(1, bits_ref.shape[0]):
        all_kept = all_kept * bits_ref[section].astype(F32)
    kept_ref[...] = all_kept

    def visit(micro, block, owner, slot):
        lanes = pl.ds(pl.multiple_of(block * rows, rows), rows)
        meta_ref[owner, pl.ds(mask_base + slot, 1), :] = kept_ref[pl.ds(micro * blocks + block, 1), :]

        @pl.when(slot >= early)
        def _():
            late = slot - early
            out_ref[owner, pl.ds(pl.multiple_of(late * rows, rows), rows), :] = values_ref[micro * blocks + block]
            keys = keys_ref[pl.ds(micro, 1), lanes]
            groups = groups_ref[pl.ds(micro, 1), lanes]
            base = late * 4
            meta_ref[owner, pl.ds(base, 1), :] = (keys >> 7).astype(F32)
            meta_ref[owner, pl.ds(base + 1, 1), :] = (keys & 127).astype(F32)
            meta_ref[owner, pl.ds(base + 2, 1), :] = (groups >> 7).astype(F32)
            meta_ref[owner, pl.ds(base + 3, 1), :] = (groups & 127).astype(F32)

    walk_blocks(dest_ref, count_ref, owners, batches, blocks, visit)
    out_ref[:, late_slots * rows :, :] = meta_ref[...].astype(BF16)


def build_table(keys_ref, values_ref, out_ref):
    columns = values_ref.shape[1]
    chunks, lanes = keys_ref.shape
    tiles = out_ref.shape[0] // lanes
    sub = lax.broadcasted_iota(jnp.int32, (lanes, lanes), 0)
    low, high = [], []
    for chunk in range(chunks):
        row = keys_ref[pl.ds(chunk, 1), :]
        low.append(jnp.where(sub == (row & (lanes - 1)), 1.0, 0.0).astype(BF16))
        high.append(row >> 7)

    def tile_step(tile, carry):
        hot = [
            low[chunk] * jnp.broadcast_to(jnp.where(high[chunk] == tile, 1.0, 0.0), (lanes, lanes)).astype(BF16)
            for chunk in range(chunks)
        ]
        total = jnp.dot(jnp.concatenate(hot, axis=1), values_ref[...], preferred_element_type=F32)
        head = total.astype(BF16)
        place = pl.ds(pl.multiple_of(tile * lanes, lanes), lanes)
        out_ref[place, :columns] = head
        out_ref[place, columns:] = (total - head.astype(F32)).astype(BF16)
        return carry

    lax.fori_loop(0, tiles, tile_step, 0)


def join_rows(values, meta_columns, table_ref, weights):
    for weight in weights:
        half = jnp.dot(values, weight, preferred_element_type=F32) * 0.5
        values = (values.astype(F32) + (half + half * jnp.tanh(half))).astype(BF16)
    columns = values.shape[1]
    tiles = table_ref.shape[0] // 128
    hot = []
    for high, low in meta_columns:
        rows = high.shape[0]
        lane = lax.broadcasted_iota(jnp.int32, (rows, 128), 1).astype(F32)
        one = jnp.where(lane == low, 1.0, 0.0)
        hot.append(jnp.concatenate([jnp.where(high == float(t), one, 0.0).astype(BF16) for t in range(tiles)], axis=1))
    found = jnp.dot(jnp.concatenate(hot, axis=0), table_ref[...], preferred_element_type=F32)
    matched = found[:, :columns] + found[:, columns:]
    return (values.astype(F32) * matched).astype(BF16)


def pick_weights(weights_ref, home):
    sections = weights_ref.shape[0]
    return [weights_ref[lax.rem(home + j, sections)] for j in range(sections)]


def join_first(early, rows, home_ref, first_ref, weights_ref, table_ref, out_ref):
    weights = pick_weights(weights_ref, home_ref[0])

    def step(source, carry):
        meta = first_ref[source, early * rows :, :].astype(F32)
        turned = meta.T
        pairs = [(turned[:, 4 * j : 4 * j + 1], turned[:, 4 * j + 1 : 4 * j + 2]) for j in range(early)]
        out_ref[source] = join_rows(first_ref[source, : early * rows, :], pairs, table_ref, weights)
        return carry

    lax.fori_loop(0, first_ref.shape[0], step, 0)


def group_hot(groups, high, low, kept):
    group = jnp.where(kept > 0.5, high * 128.0 + low, -1.0)
    sub = lax.broadcasted_iota(jnp.int32, (groups, group.shape[1]), 0).astype(F32)
    return jnp.where(sub == group, 1.0, 0.0).astype(BF16)


def join_last(early, rows, home_ref, first_ref, last_ref, joined_ref, weights_ref, table_ref, out_ref):
    weights = pick_weights(weights_ref, home_ref[0])
    groups = out_ref.shape[0]
    late = (last_ref.shape[1] - META) // rows
    out_ref[...] = jnp.zeros_like(out_ref)

    def step(source, carry):
        early_meta = first_ref[source, early * rows :, :].astype(F32)
        late_meta = last_ref[source, late * rows :, :].astype(F32)
        kept = late_meta[4 * late : 4 * late + early + late]
        turned = late_meta.T
        pairs = [(turned[:, 4 * j : 4 * j + 1], turned[:, 4 * j + 1 : 4 * j + 2]) for j in range(late)]
        fresh = join_rows(last_ref[source, : late * rows, :], pairs, table_ref, weights)
        hot = [
            group_hot(groups, early_meta[4 * j + 2 : 4 * j + 3], early_meta[4 * j + 3 : 4 * j + 4], kept[j : j + 1])
            for j in range(early)
        ] + [
            group_hot(
                groups, late_meta[4 * j + 2 : 4 * j + 3], late_meta[4 * j + 3 : 4 * j + 4], kept[early + j : early + j + 1]
            )
            for j in range(late)
        ]
        joined = jnp.concatenate([joined_ref[source], fresh], axis=0)
        out_ref[...] += jnp.dot(jnp.concatenate(hot, axis=1), joined, preferred_element_type=F32)
        return carry

    lax.fori_loop(0, first_ref.shape[0], step, 0)


def unpack_bits(bit_words):
    shifts = jnp.arange(16, dtype=jnp.int32)
    spread = jnp.right_shift(bit_words[..., None], shifts) & 1
    return spread.reshape(bit_words.shape[:-1] + (bit_words.shape[-1] * 16,))


def local(
    probe_values,
    probe_keys,
    group_ids,
    block_dest,
    filter_bits,
    section_weights,
    build_keys,
    build_values,
):
    sections = lax.axis_size("section")
    owners = lax.axis_size("owner")
    batches, block_count = block_dest.shape[:2]
    columns = probe_values.shape[2]
    rows = probe_values.shape[1] // block_count
    groups_all = GRP_DEV * sections * owners
    slots = batches * CAP
    late = 1
    early = slots - late

    dest = block_dest.reshape(batches, block_count)
    blocks = probe_values.reshape(batches * block_count, rows, columns)
    first = pl.pallas_call(
        functools.partial(pack_first, early, rows),
        out_shape=jax.ShapeDtypeStruct((owners, early * rows + META, columns), BF16),
        in_specs=[smem(), vmem(), vmem(), vmem()],
        out_specs=vmem(),
        scratch_shapes=[pltpu.VMEM((owners, META, columns), F32), pltpu.SMEM((owners,), jnp.int32)],
        compiler_params=params(),
        name="pack_first",
    )(dest, blocks, probe_keys, group_ids)
    first = lax.all_to_all(first, "owner", split_axis=0, concat_axis=0, tiled=True)

    bits = unpack_bits(filter_bits[0]).astype(BF16).reshape(sections, batches * block_count, rows)
    shared = jnp.concatenate([jnp.broadcast_to(section_weights, (sections, columns, columns)), bits], axis=1)
    shared = lax.all_to_all(shared, "section", split_axis=0, concat_axis=0, tiled=True)
    weights = shared[:, :columns]
    bits = shared[:, columns:]

    table = pl.pallas_call(
        build_table,
        out_shape=jax.ShapeDtypeStruct((KEYS_OWN, 2 * columns), BF16),
        in_specs=[vmem(), vmem()],
        out_specs=vmem(),
        compiler_params=params(),
        cost_estimate=pl.CostEstimate(flops=2 * KEYS_OWN * build_keys.shape[0] * columns, bytes_accessed=2**21, transcendentals=0),
        name="build_table",
    )(build_keys.reshape(-1, 128), build_values)

    last = pl.pallas_call(
        functools.partial(pack_last, early, rows),
        out_shape=jax.ShapeDtypeStruct((owners, late * rows + META, columns), BF16),
        in_specs=[smem(), vmem(), vmem(), vmem(), vmem()],
        out_specs=vmem(),
        scratch_shapes=[
            pltpu.VMEM((owners, META, columns), F32),
            pltpu.VMEM((batches * block_count, rows), F32),
            pltpu.SMEM((owners,), jnp.int32),
        ],
        compiler_params=params(),
        name="pack_last",
    )(dest, blocks, probe_keys, group_ids, bits)
    last = lax.all_to_all(last, "owner", split_axis=0, concat_axis=0, tiled=True)

    home = lax.axis_index("section").astype(jnp.int32).reshape(1)
    joined = pl.pallas_call(
        functools.partial(join_first, early, rows),
        out_shape=jax.ShapeDtypeStruct((owners, early * rows, columns), BF16),
        in_specs=[smem(), vmem(), vmem(), vmem()],
        out_specs=vmem(),
        compiler_params=params(),
        cost_estimate=pl.CostEstimate(
            flops=2 * KEYS_OWN * owners * early * rows * 2 * columns, bytes_accessed=2**21, transcendentals=0
        ),
        name="join_first",
    )(home, first, weights, table)
    sums = pl.pallas_call(
        functools.partial(join_last, early, rows),
        out_shape=jax.ShapeDtypeStruct((groups_all, columns), F32),
        in_specs=[smem(), vmem(), vmem(), vmem(), vmem(), vmem()],
        out_specs=vmem(),
        compiler_params=params(),
        cost_estimate=pl.CostEstimate(
            flops=2 * KEYS_OWN * owners * late * rows * 2 * columns, bytes_accessed=2**21, transcendentals=0
        ),
        name="join_last",
    )(home, first, last, joined, weights, table)
    parts = sums.reshape(sections * owners, GRP_DEV, columns)
    parts = lax.all_to_all(parts, ("section", "owner"), split_axis=0, concat_axis=0, tiled=True)
    return jnp.sum(parts, axis=0)


def solution(mesh):
    placed = (
        P("section", "owner", None),
        P("section", "owner"),
        P("section", "owner"),
        P("section", "owner", None),
        P("section", None, "owner"),
        P("section", None, None),
        P("owner"),
        P("owner", None),
    )
    return jax.shard_map(
        local, mesh=mesh, in_specs=placed, out_specs=P(("section", "owner"), None), check_vma=False
    )
```

```python
import functools
import math

import jax
import jax.numpy as jnp
from jax import lax
from jax.experimental import pallas as pl
from jax.experimental.pallas import tpu as pltpu
from jax.sharding import PartitionSpec as P

CAP = 2
KEYS_OWN = 2048
GRP_DEV = 4
FIELDS = 4
BF16 = jnp.bfloat16
F32 = jnp.float32
I32 = jnp.int32


def run(kernel, name, ins, outs, scratch=(), scalars=0, flops=0):
    several = isinstance(outs, list)
    shapes = [jax.ShapeDtypeStruct(shape, dtype) for shape, dtype in (outs if several else [outs])]
    held = [x for x in ins[scalars:]] + shapes
    size = sum(math.prod(x.shape) * x.dtype.itemsize for x in held)
    for entry in scratch:
        size += 2 * math.prod(getattr(entry, "shape", ())) * 4
    place = pl.BlockSpec(memory_space=pltpu.VMEM)
    return pl.pallas_call(
        kernel,
        out_shape=shapes if several else shapes[0],
        in_specs=[pl.BlockSpec(memory_space=pltpu.SMEM)] * scalars + [place] * (len(ins) - scalars),
        out_specs=[place] * len(shapes) if several else place,
        scratch_shapes=list(scratch),
        compiler_params=pltpu.CompilerParams(vmem_limit_bytes=size + 4 * 2**20),
        cost_estimate=pl.CostEstimate(flops=flops, bytes_accessed=size, transcendentals=0) if flops else None,
        name=name,
    )(*ins)


def walk_blocks(dest_ref, count_ref, owners, visit):
    batches, blocks = dest_ref.shape

    def clear(owner, carry):
        count_ref[owner] = 0
        return carry

    lax.fori_loop(0, owners, clear, 0)
    for micro in range(batches):

        def step(block, carry, micro=micro):
            owner = dest_ref[micro, block]
            slot = count_ref[owner]
            count_ref[owner] = slot + 1
            visit(micro, block, owner, slot)
            return carry

        lax.fori_loop(0, blocks, step, 0, unroll=min(blocks, 8))


def pack_blocks(slots, dest_ref, values_ref, keys_ref, groups_ref, out_ref, meta_ref, count_ref):
    owners = out_ref.shape[0]
    blocks = dest_ref.shape[1]
    rows = values_ref.shape[1]
    meta_ref[...] = jnp.zeros_like(meta_ref)
    out_ref[...] = jnp.zeros_like(out_ref)

    def visit(micro, block, owner, slot):
        lanes = pl.ds(pl.multiple_of(block * rows, rows), rows)
        out_ref[owner, pl.ds(pl.multiple_of(slot * rows, rows), rows), :] = values_ref[micro * blocks + block]
        keys = keys_ref[pl.ds(micro, 1), lanes]
        groups = groups_ref[pl.ds(micro, 1), lanes]
        for field, part in enumerate((keys >> 7, keys & 127, groups >> 7, groups & 127)):
            meta_ref[owner, pl.ds(field * slots + slot, 1), :] = part.astype(F32)

    walk_blocks(dest_ref, count_ref, owners, visit)
    out_ref[:, slots * rows :, :] = meta_ref[...].astype(BF16)


def build_table(keys_ref, values_ref, out_ref):
    chunks, lanes = keys_ref.shape
    tiles = out_ref.shape[0] // lanes
    sub = lax.broadcasted_iota(I32, (lanes, lanes), 0)
    low, high = [], []
    for chunk in range(chunks):
        row = keys_ref[pl.ds(chunk, 1), :]
        low.append(jnp.where(sub == (row & (lanes - 1)), 1.0, 0.0).astype(BF16))
        high.append(row >> 7)

    def tile_step(tile, carry):
        hot = [
            low[chunk] * jnp.broadcast_to(jnp.where(high[chunk] == tile, 1.0, 0.0), (lanes, lanes)).astype(BF16)
            for chunk in range(chunks)
        ]
        place = pl.ds(pl.multiple_of(tile * lanes, lanes), lanes)
        out_ref[place, :] = jnp.dot(jnp.concatenate(hot, axis=1), values_ref[...], preferred_element_type=F32)
        return carry

    lax.fori_loop(0, tiles, tile_step, 0)


def place_bits(sections, dest_ref, home_ref, *refs):
    shared, (weights_ref, out_ref, kept_ref, count_ref) = refs[:sections], refs[sections:]
    owners = out_ref.shape[0]
    batches, blocks = dest_ref.shape
    columns = weights_ref.shape[1]
    home = home_ref[0]
    own = pl.ds(pl.multiple_of(columns + home * batches * blocks, batches * blocks), batches * blocks)
    kept = shared[0][own, :].astype(F32)
    for ref in shared[1:]:
        kept = kept * ref[own, :].astype(F32)
    kept_ref[...] = kept
    for k, ref in enumerate(shared):
        weights_ref[home_ref[1 + k]] = ref[:columns, :]
    out_ref[...] = jnp.zeros_like(out_ref)

    def visit(micro, block, owner, slot):
        out_ref[owner, pl.ds(slot, 1), :] = kept_ref[pl.ds(micro * blocks + block, 1), :]

    walk_blocks(dest_ref, count_ref, owners, visit)


def join_blocks(slots, first_ref, weights_ref, table_ref, out_ref, keys_ref, found_ref, places_ref, sem):
    owners, columns = first_ref.shape[0], first_ref.shape[2]
    span = out_ref.shape[1]
    group = math.gcd(owners, 2)
    meta = first_ref[:, span : span + 2 * slots, :].astype(F32)
    keys_ref[...] = (meta[:, :slots] * 128.0 + meta[:, slots:]).astype(I32)
    copy = pltpu.make_async_copy(keys_ref, places_ref, sem)
    copy.start()
    weights = [weights_ref[j] for j in range(weights_ref.shape[0])]
    copy.wait()

    def step(turn, carry):
        base = turn * group
        values = first_ref[pl.ds(base, group), :span, :].reshape(group * span, columns)
        for source in range(group):
            for slot in range(slots):
                for row in range(span // slots):
                    place = places_ref[base + source, slot, row]
                    found_ref[pl.ds(source * span + slot * (span // slots) + row, 1), :] = table_ref[pl.ds(place, 1), :]
        for weight in weights:
            half = jnp.dot(values, weight, preferred_element_type=F32) * 0.5
            values = (values.astype(F32) + (half + half * jnp.tanh(half))).astype(BF16)
        joined = (values.astype(F32) * found_ref[...]).astype(BF16)
        out_ref[pl.ds(base, group)] = joined.reshape(group, span, columns)
        return carry

    lax.fori_loop(0, owners // group, step, 0)


def sum_groups(slots, first_ref, kept_ref, joined_ref, out_ref):
    owners, span, columns = joined_ref.shape
    groups = out_ref.shape[0]
    rows = span // slots
    step_size = math.gcd(owners, 8) if groups <= 128 else 1
    out_ref[...] = jnp.zeros_like(out_ref)
    sub = lax.broadcasted_iota(I32, (groups, rows), 0).astype(F32)

    def step(turn, carry):
        hot = []
        for source in range(step_size):
            at = turn * step_size + source
            meta = first_ref[at, span:, :].astype(F32)
            group = meta[2 * slots : 3 * slots] * 128.0 + meta[3 * slots : 4 * slots]
            group = jnp.where(kept_ref[at, :slots, :] > 0.5, group, -1.0)
            hot += [jnp.where(sub == group[j : j + 1], 1.0, 0.0).astype(BF16) for j in range(slots)]
        joined = joined_ref[pl.ds(turn * step_size, step_size)].reshape(step_size * span, columns)
        out_ref[...] += jnp.dot(jnp.concatenate(hot, axis=1), joined, preferred_element_type=F32)
        return carry

    lax.fori_loop(0, owners // step_size, step, 0)


def unpack_bits(bit_words):
    shifts = jnp.arange(16, dtype=jnp.int32)
    spread = jnp.right_shift(bit_words[..., None], shifts) & 1
    return spread.reshape(bit_words.shape[:-1] + (bit_words.shape[-1] * 16,))


def local(
    probe_values,
    probe_keys,
    group_ids,
    block_dest,
    filter_bits,
    section_weights,
    build_keys,
    build_values,
):
    sections = lax.axis_size("section")
    owners = lax.axis_size("owner")
    home = lax.axis_index("section").astype(I32)
    batches, block_count = block_dest.shape[:2]
    columns = probe_values.shape[2]
    rows = probe_values.shape[1] // block_count
    groups_all = GRP_DEV * sections * owners
    slots = batches * CAP
    span = slots * rows

    dest = block_dest.reshape(batches, block_count)
    blocks = probe_values.reshape(batches * block_count, rows, columns)
    counts = pltpu.SMEM((owners,), I32)
    first = run(
        functools.partial(pack_blocks, slots),
        "pack_blocks",
        [dest, blocks, probe_keys, group_ids],
        ((owners, span + FIELDS * slots, columns), BF16),
        [pltpu.VMEM((owners, FIELDS * slots, columns), F32), counts],
        scalars=1,
    )
    first = lax.all_to_all(first, "owner", split_axis=0, concat_axis=0, tiled=True)

    bits = unpack_bits(filter_bits[0]).astype(BF16).reshape(-1, rows)
    shared = jnp.concatenate([section_weights[0], bits], axis=0)
    paired = sections & (sections - 1) == 0

    def partner(index, k):
        return index ^ k if paired else (index - k) % sections

    received = [shared] + [
        lax.ppermute(shared, "section", [(partner(i, k), i) for i in range(sections)]) for k in range(1, sections)
    ]
    order = jnp.stack([home] + [lax.rem(partner(home, k) - home + sections, sections) for k in range(sections)])
    table = run(
        build_table,
        "build_table",
        [build_keys.reshape(-1, 128), build_values],
        ((KEYS_OWN, columns), F32),
        flops=2 * KEYS_OWN * build_keys.shape[0] * columns,
    )
    weights, kept = run(
        functools.partial(place_bits, sections),
        "place_bits",
        [dest, order] + received,
        [((sections, columns, columns), BF16), ((owners, 8, rows), F32)],
        [pltpu.VMEM((batches * block_count, rows), F32), counts],
        scalars=2,
    )
    kept, table = lax.optimization_barrier((kept, table))
    kept = lax.all_to_all(kept, "owner", split_axis=0, concat_axis=0, tiled=True)

    group = math.gcd(owners, 2)
    joined = run(
        functools.partial(join_blocks, slots),
        "join_blocks",
        [first, weights, table],
        ((owners, span, columns), BF16),
        [
            pltpu.VMEM((owners, slots, rows), I32),
            pltpu.VMEM((group * span, columns), F32),
            pltpu.SMEM((owners, slots, rows), I32),
            pltpu.SemaphoreType.DMA,
        ],
        flops=2 * KEYS_OWN * owners * span * columns,
    )
    sums = run(
        functools.partial(sum_groups, slots),
        "sum_groups",
        [first, kept, joined],
        ((groups_all, columns), F32),
        flops=2 * groups_all * owners * span * columns,
    )
    parts = sums.reshape(sections * owners, GRP_DEV, columns)
    parts = lax.all_to_all(parts, ("section", "owner"), split_axis=0, concat_axis=0, tiled=True)
    return jnp.sum(parts, axis=0)


def solution(mesh):
    placed = (
        P("section", "owner", None),
        P("section", "owner"),
        P("section", "owner"),
        P("section", "owner", None),
        P("section", None, "owner"),
        P("section", None, None),
        P("owner"),
        P("owner", None),
    )
    return jax.shard_map(
        local, mesh=mesh, in_specs=placed, out_specs=P(("section", "owner"), None), check_vma=False
    )
```

```python
import functools
import math

import jax
import jax.numpy as jnp
from jax import lax
from jax.experimental import pallas as pl
from jax.experimental.pallas import tpu as pltpu
from jax.sharding import PartitionSpec as P

CAP = 2
KEYS_OWN = 2048
GRP_DEV = 4
FIELDS = 4
BF16 = jnp.bfloat16
F32 = jnp.float32
I32 = jnp.int32


def run(kernel, name, ins, outs, scratch=(), scalars=(), flops=0, away=False):
    several = isinstance(outs, list)
    shapes = [jax.ShapeDtypeStruct(shape, dtype) for shape, dtype in (outs if several else [outs])]
    held = shapes + [x for k, x in enumerate(ins) if k not in scalars and not away]
    size = sum(math.prod(x.shape) * x.dtype.itemsize for x in held)
    for entry in scratch:
        size += 2 * math.prod(getattr(entry, "shape", ())) * 4
    place = pl.BlockSpec(memory_space=pltpu.VMEM)
    spaces = [pltpu.HBM if away else pltpu.SMEM if k in scalars else pltpu.VMEM for k in range(len(ins))]
    return pl.pallas_call(
        kernel,
        out_shape=shapes if several else shapes[0],
        in_specs=[pl.BlockSpec(memory_space=space) for space in spaces],
        out_specs=[place] * len(shapes) if several else place,
        scratch_shapes=list(scratch),
        compiler_params=pltpu.CompilerParams(vmem_limit_bytes=60 * 2**20 if away else min(size + 4 * 2**20, 60 * 2**20)),
        cost_estimate=pl.CostEstimate(flops=flops, bytes_accessed=size, transcendentals=0) if flops else None,
        name=name,
    )(*ins)


def walk_blocks(dest_ref, count_ref, owners, visit):
    batches, blocks = dest_ref.shape

    def clear(owner, carry):
        count_ref[owner] = 0
        return carry

    lax.fori_loop(0, owners, clear, 0)
    for micro in range(batches):

        def step(block, carry, micro=micro):
            owner = dest_ref[micro, block]
            slot = count_ref[owner]
            count_ref[owner] = slot + 1
            visit(micro, block, owner, slot)
            return carry

        lax.fori_loop(0, blocks, step, 0, unroll=min(blocks, 8))


def put_block(slots, field_base, source, owner_at, slot, out_ref, meta_ref):
    values, keys, groups = source
    rows = values.shape[0]
    out_ref[owner_at, pl.ds(pl.multiple_of(slot * rows, rows), rows), :] = values
    for field, part in enumerate((keys >> 7, keys & 127, groups >> 7, groups & 127)):
        meta_ref[owner_at, pl.ds(field_base + field * slots + slot, 1), :] = part.astype(F32)


def pack_first(early, *refs):
    sources, (out_ref, dest_ref, values_ref, keys_ref, groups_ref, meta_ref, count_ref, sems) = refs[:4], refs[4:]
    owners = out_ref.shape[0]
    blocks = dest_ref.shape[1]
    rows = values_ref.shape[1]
    copies = [
        pltpu.make_async_copy(source, target, sems.at[k])
        for k, (source, target) in enumerate(zip(sources, (dest_ref, values_ref, keys_ref, groups_ref)))
    ]
    for copy in copies:
        copy.start()
    meta_ref[...] = jnp.zeros_like(meta_ref)
    out_ref[...] = jnp.zeros_like(out_ref)
    for copy in copies:
        copy.wait()

    def visit(micro, block, owner, slot):
        @pl.when(slot < early)
        def _():
            lanes = pl.ds(pl.multiple_of(block * rows, rows), rows)
            source = (values_ref[micro * blocks + block], keys_ref[pl.ds(micro, 1), lanes], groups_ref[pl.ds(micro, 1), lanes])
            put_block(early, 0, source, owner, slot, out_ref, meta_ref)

    walk_blocks(dest_ref, count_ref, owners, visit)
    out_ref[:, early * rows :, :] = meta_ref[...].astype(BF16)


def build_table(keys_ref, values_ref, out_ref, wide_ref):
    chunks, lanes = keys_ref.shape
    columns = values_ref.shape[1]
    tiles = out_ref.shape[0] // lanes // 2
    sub = lax.broadcasted_iota(I32, (lanes, lanes), 0)
    keys = keys_ref[...]
    upper = jnp.where(keys >= tiles * lanes, 1.0, 0.0).T
    middle = (keys >> 7) & (tiles - 1)
    low = []
    for chunk in range(chunks):
        low.append(jnp.where(sub == (keys[chunk : chunk + 1] & (lanes - 1)), 1.0, 0.0).astype(BF16))
        flag = jnp.broadcast_to(upper[:, chunk : chunk + 1], (lanes, columns)).astype(BF16)
        part = values_ref[chunk * lanes : (chunk + 1) * lanes, :]
        high_part = part * flag
        wide_ref[chunk * lanes : (chunk + 1) * lanes, :columns] = part - high_part
        wide_ref[chunk * lanes : (chunk + 1) * lanes, columns:] = high_part

    def tile_step(tile, carry):
        here = jnp.where(middle == tile, 1.0, 0.0)
        hot = [low[chunk] * jnp.broadcast_to(here[chunk : chunk + 1], (lanes, lanes)).astype(BF16) for chunk in range(chunks)]
        total = jnp.dot(jnp.concatenate(hot, axis=1), wide_ref[...], preferred_element_type=F32)
        out_ref[pl.ds(pl.multiple_of(tile * lanes, lanes), lanes), :] = total[:, :columns]
        out_ref[pl.ds(pl.multiple_of((tiles + tile) * lanes, lanes), lanes), :] = total[:, columns:]
        return carry

    lax.fori_loop(0, tiles, tile_step, 0)


def pack_last(sections, paired, early, late, scalar_ref, *refs):
    shared, (values_ref, keys_ref, groups_ref, dest_ref, table_ref), refs = refs[:sections], refs[sections : sections + 5], refs[sections + 5 :]
    weights_ref, outs, (buffer_ref, meta_ref, kept_ref, count_ref) = refs[0], refs[1:-4], refs[-4:]
    owners = buffer_ref.shape[0]
    batches, blocks = dest_ref.shape
    rows = values_ref.shape[1]
    columns = weights_ref.shape[1]
    me, home = scalar_ref[sections], scalar_ref[sections + 1]
    count = batches * blocks
    own = pl.ds(pl.multiple_of(columns + home * count, count), count)
    kept = shared[0][own, :].astype(F32)
    for ref in shared[1:]:
        kept = kept * ref[own, :].astype(F32)
    kept_ref[...] = kept
    for k, ref in enumerate(shared):
        weights_ref[scalar_ref[k]] = ref[:columns, :]
    meta_ref[...] = jnp.zeros_like(meta_ref)
    buffer_ref[...] = jnp.zeros_like(buffer_ref)

    def visit(micro, block, owner, slot):
        at = owner ^ me if paired else owner
        meta_ref[at, pl.ds(FIELDS * late + slot, 1), :] = kept_ref[pl.ds(micro * blocks + block, 1), :]

        @pl.when(slot >= early)
        def _():
            lanes = pl.ds(pl.multiple_of(block * rows, rows), rows)
            source = (values_ref[micro * blocks + block], keys_ref[pl.ds(micro, 1), lanes], groups_ref[pl.ds(micro, 1), lanes])
            put_block(late, 0, source, at, slot - early, buffer_ref, meta_ref)

    walk_blocks(dest_ref, count_ref, owners, visit)
    buffer_ref[:, late * rows :, :] = meta_ref[...].astype(BF16)
    if len(outs) == 1:
        outs[0][...] = buffer_ref[...]
    else:
        for k, out in enumerate(outs):
            out[...] = buffer_ref[k]


def chain(values, weights):
    for weight in weights:
        half = jnp.dot(values, weight, preferred_element_type=F32) * 0.5
        values = (values.astype(F32) + (half + half * jnp.tanh(half))).astype(BF16)
    return values


def fetch_keys(meta_ref, start, slots, keys_ref, places_ref, sem):
    meta = meta_ref[:, start : start + 2 * slots, :].astype(F32)
    keys_ref[...] = (meta[:, :slots] * 128.0 + meta[:, slots:]).astype(I32)
    return pltpu.make_async_copy(keys_ref, places_ref, sem)


def find_rows(source, slots, at, rows, places_ref, table_ref, found_ref):
    for slot in range(slots):
        for row in range(rows):
            place = places_ref[source, slot, row]
            found_ref[pl.ds(at + slot * rows + row, 1), :] = table_ref[pl.ds(place, 1), :]


def join_first(slots, first_ref, weights_ref, table_ref, out_ref, keys_ref, found_ref, places_ref, sem):
    owners, columns = first_ref.shape[0], first_ref.shape[2]
    span = out_ref.shape[1]
    group = math.gcd(owners, 2)
    copy = fetch_keys(first_ref, span, slots, keys_ref, places_ref, sem)
    copy.start()
    weights = [weights_ref[j] for j in range(weights_ref.shape[0])]
    copy.wait()

    def step(turn, carry):
        base = turn * group
        values = first_ref[pl.ds(base, group), :span, :].reshape(group * span, columns)
        for source in range(group):
            find_rows(base + source, slots, source * span, span // slots, places_ref, table_ref, found_ref)
        joined = (chain(values, weights).astype(F32) * found_ref[...]).astype(BF16)
        out_ref[pl.ds(base, group)] = joined.reshape(group, span, columns)
        return carry

    lax.fori_loop(0, owners // group, step, 0)


def group_hot(slots, meta, kept, sub):
    group = meta[2 * slots : 3 * slots] * 128.0 + meta[3 * slots : 4 * slots]
    group = jnp.where(kept > 0.5, group, -1.0)
    return [jnp.where(sub == group[j : j + 1], 1.0, 0.0).astype(BF16) for j in range(slots)]


def join_last(paired, early, late, scalar_ref, first_ref, joined_ref, weights_ref, table_ref, *refs):
    parts, (out_ref, buffer_ref, keys_ref, found_ref, places_ref, sem) = refs[:-6], refs[-6:]
    owners, span, columns = joined_ref.shape
    groups = out_ref.shape[0]
    rows = span // early
    me = scalar_ref[weights_ref.shape[0]]
    if len(parts) == 1:
        buffer_ref[...] = parts[0][...]
    else:
        for k, part in enumerate(parts):
            buffer_ref[me ^ k] = part[...]
    copy = fetch_keys(buffer_ref, late * rows, late, keys_ref, places_ref, sem)
    copy.start()
    weights = [weights_ref[j] for j in range(weights_ref.shape[0])]
    step_size = math.gcd(owners, 8) if groups <= 128 else 1
    out_ref[...] = jnp.zeros_like(out_ref)
    sub = lax.broadcasted_iota(I32, (groups, rows), 0).astype(F32)
    copy.wait()

    def step(turn, carry):
        base = turn * step_size
        values = buffer_ref[pl.ds(base, step_size), : late * rows, :].reshape(step_size * late * rows, columns)
        hot, fresh_hot = [], []
        for source in range(step_size):
            meta = first_ref[base + source, span:, :].astype(F32)
            fresh = buffer_ref[base + source, late * rows :, :].astype(F32)
            kept = fresh[FIELDS * late : FIELDS * late + early + late]
            hot += group_hot(early, meta, kept[:early], sub)
            fresh_hot += group_hot(late, fresh, kept[early:], sub)
            find_rows(base + source, late, source * late * rows, rows, places_ref, table_ref, found_ref)
        total = jnp.dot(
            jnp.concatenate(hot, axis=1),
            joined_ref[pl.ds(base, step_size)].reshape(step_size * span, columns),
            preferred_element_type=F32,
        )
        joined = (chain(values, weights).astype(F32) * found_ref[...]).astype(BF16)
        total += jnp.dot(jnp.concatenate(fresh_hot, axis=1), joined, preferred_element_type=F32)
        out_ref[...] += total
        return carry

    lax.fori_loop(0, owners // step_size, step, 0)


def unpack_bits(bit_words):
    shifts = jnp.arange(16, dtype=jnp.int32)
    spread = jnp.right_shift(bit_words[..., None], shifts) & 1
    return spread.reshape(bit_words.shape[:-1] + (bit_words.shape[-1] * 16,))


def local(
    probe_values,
    probe_keys,
    group_ids,
    block_dest,
    filter_bits,
    section_weights,
    build_keys,
    build_values,
):
    sections = lax.axis_size("section")
    owners = lax.axis_size("owner")
    home = lax.axis_index("section").astype(I32)
    batches, block_count = block_dest.shape[:2]
    columns = probe_values.shape[2]
    rows = probe_values.shape[1] // block_count
    groups_all = GRP_DEV * sections * owners
    slots = batches * CAP
    late = 1
    early = slots - late
    tile = 16
    early_meta = -(-FIELDS * early // tile) * tile
    late_meta = -(-(FIELDS * late + slots) // tile) * tile

    dest = block_dest.reshape(batches, block_count)
    blocks = probe_values.reshape(batches * block_count, rows, columns)
    counts = pltpu.SMEM((owners,), I32)
    first = run(
        functools.partial(pack_first, early),
        "pack_first",
        [dest, blocks, probe_keys, group_ids],
        ((owners, early * rows + early_meta, columns), BF16),
        [
            pltpu.SMEM(dest.shape, I32),
            pltpu.VMEM(blocks.shape, BF16),
            pltpu.VMEM(probe_keys.shape, I32),
            pltpu.VMEM(group_ids.shape, I32),
            pltpu.VMEM((owners, early_meta, columns), F32),
            counts,
            pltpu.SemaphoreType.DMA((4,)),
        ],
        away=True,
    )
    first = lax.all_to_all(first, "owner", split_axis=0, concat_axis=0, tiled=True)

    bits = unpack_bits(filter_bits[0]).astype(BF16).reshape(-1, rows)
    shared = jnp.concatenate([section_weights[0], bits], axis=0)
    paired = sections & (sections - 1) == 0

    def partner(index, k):
        return index ^ k if paired else (index - k) % sections

    received = [shared] + [
        lax.ppermute(shared, "section", [(partner(i, k), i) for i in range(sections)]) for k in range(1, sections)
    ]
    scalars = jnp.stack(
        [lax.rem(partner(home, k) - home + sections, sections) for k in range(sections)]
        + [lax.axis_index("owner").astype(I32), home]
    )
    table = run(
        build_table,
        "build_table",
        [build_keys.reshape(-1, 128), build_values],
        ((KEYS_OWN, columns), F32),
        [pltpu.VMEM((build_values.shape[0], 2 * columns), BF16)],
        flops=2 * KEYS_OWN * build_keys.shape[0] * columns,
    )
    few = owners <= 8 and owners & (owners - 1) == 0
    part = (late * rows + late_meta, columns)
    weights, *parts = run(
        functools.partial(pack_last, sections, few, early, late),
        "pack_last",
        [scalars] + received + [blocks, probe_keys, group_ids, dest, table],
        [((sections, columns, columns), BF16)] + ([(part, BF16)] * owners if few else [((owners, *part), BF16)]),
        [
            pltpu.VMEM((owners, *part), BF16),
            pltpu.VMEM((owners, late_meta, columns), F32),
            pltpu.VMEM((batches * block_count, rows), F32),
            counts,
        ],
        scalars=(0, 1 + sections + 3),
    )
    if few:
        parts = [parts[0]] + [
            lax.ppermute(parts[k], "owner", [(i, i ^ k) for i in range(owners)]) for k in range(1, owners)
        ]
    else:
        parts = [lax.all_to_all(parts[0], "owner", split_axis=0, concat_axis=0, tiled=True)]

    group = math.gcd(owners, 2)
    joined = run(
        functools.partial(join_first, early),
        "join_first",
        [first, weights, table],
        ((owners, early * rows, columns), BF16),
        [
            pltpu.VMEM((owners, early, rows), I32),
            pltpu.VMEM((group * early * rows, columns), F32),
            pltpu.SMEM((owners, early, rows), I32),
            pltpu.SemaphoreType.DMA,
        ],
        flops=2 * KEYS_OWN * owners * early * rows * columns,
    )
    sums = run(
        functools.partial(join_last, few, early, late),
        "join_last",
        [scalars, first, joined, weights, table] + parts,
        ((groups_all, columns), F32),
        [
            pltpu.VMEM((owners, *part), BF16),
            pltpu.VMEM((owners, late, rows), I32),
            pltpu.VMEM((owners * late * rows if groups_all <= 128 else late * rows, columns), F32),
            pltpu.SMEM((owners, late, rows), I32),
            pltpu.SemaphoreType.DMA,
        ],
        scalars=(0,),
        flops=2 * groups_all * owners * slots * rows * columns,
    )
    parts = sums.reshape(sections * owners, GRP_DEV, columns)
    parts = lax.all_to_all(parts, ("section", "owner"), split_axis=0, concat_axis=0, tiled=True)
    return jnp.sum(parts, axis=0)


def solution(mesh):
    placed = (
        P("section", "owner", None),
        P("section", "owner"),
        P("section", "owner"),
        P("section", "owner", None),
        P("section", None, "owner"),
        P("section", None, None),
        P("owner"),
        P("owner", None),
    )
    return jax.shard_map(
        local, mesh=mesh, in_specs=placed, out_specs=P(("section", "owner"), None), check_vma=False
    )
```

```python
import functools
import math

import jax
import jax.numpy as jnp
from jax import lax
from jax.experimental import pallas as pl
from jax.experimental.pallas import tpu as pltpu
from jax.sharding import PartitionSpec as P


CAP = 2
KEYS_OWN = 2048
GRP_DEV = 4
FIELDS = 4
BF16 = jnp.bfloat16
F32 = jnp.float32
I32 = jnp.int32


def run(kernel, ins, outs, scratch=(), scalars=(), flops=0, away=False):
    several = isinstance(outs, list)
    shapes = [jax.ShapeDtypeStruct(shape, dtype) for shape, dtype in (outs if several else [outs])]
    held = shapes + [x for k, x in enumerate(ins) if k not in scalars and not away]
    size = sum(math.prod(x.shape) * x.dtype.itemsize for x in held)
    for entry in scratch:
        size += 2 * math.prod(getattr(entry, "shape", ())) * 4
    place = pl.BlockSpec(memory_space=pltpu.VMEM)
    spaces = [pltpu.HBM if away else pltpu.SMEM if k in scalars else pltpu.VMEM for k in range(len(ins))]
    return pl.pallas_call(
        kernel,
        out_shape=shapes if several else shapes[0],
        in_specs=[pl.BlockSpec(memory_space=space) for space in spaces],
        out_specs=[place] * len(shapes) if several else place,
        scratch_shapes=list(scratch),
        compiler_params=pltpu.CompilerParams(vmem_limit_bytes=60 * 2**20 if away else min(size + 4 * 2**20, 60 * 2**20)),
        cost_estimate=pl.CostEstimate(flops=flops, bytes_accessed=size, transcendentals=0) if flops else None,
    )(*ins)


def walk_blocks(dest_ref, count_ref, owners, visit):
    batches, blocks = dest_ref.shape

    def clear(owner, carry):
        count_ref[owner] = 0
        return carry

    lax.fori_loop(0, owners, clear, 0)
    for micro in range(batches):

        def step(block, carry, micro=micro):
            owner = dest_ref[micro, block]
            slot = count_ref[owner]
            count_ref[owner] = slot + 1
            visit(micro, block, owner, slot)
            return carry

        lax.fori_loop(0, blocks, step, 0, unroll=min(blocks, 8))


def put_block(slots, field_base, source, owner_at, slot, out_ref, meta_ref):
    values, keys, groups = source
    rows = values.shape[0]
    out_ref[owner_at, pl.ds(pl.multiple_of(slot * rows, rows), rows), :] = values
    for field, part in enumerate((keys >> 7, keys & 127, groups >> 7, groups & 127)):
        meta_ref[owner_at, pl.ds(field_base + field * slots + slot, 1), :] = part.astype(F32)


def pack_first(early, *refs):
    sources, (out_ref, dest_ref, values_ref, keys_ref, groups_ref, meta_ref, count_ref, sems) = refs[:4], refs[4:]
    owners = out_ref.shape[0]
    blocks = dest_ref.shape[1]
    rows = values_ref.shape[1]
    copies = [
        pltpu.make_async_copy(source, target, sems.at[k])
        for k, (source, target) in enumerate(zip(sources, (dest_ref, values_ref, keys_ref, groups_ref)))
    ]
    for copy in copies:
        copy.start()
    meta_ref[...] = jnp.zeros_like(meta_ref)
    out_ref[...] = jnp.zeros_like(out_ref)
    for copy in copies:
        copy.wait()

    def visit(micro, block, owner, slot):
        @pl.when(slot < early)
        def _():
            lanes = pl.ds(pl.multiple_of(block * rows, rows), rows)
            source = (values_ref[micro * blocks + block], keys_ref[pl.ds(micro, 1), lanes], groups_ref[pl.ds(micro, 1), lanes])
            put_block(early, 0, source, owner, slot, out_ref, meta_ref)

    walk_blocks(dest_ref, count_ref, owners, visit)
    out_ref[:, early * rows :, :] = meta_ref[...].astype(BF16)


def build_table(keys_ref, values_ref, out_ref, wide_ref):
    chunks, lanes = keys_ref.shape
    columns = values_ref.shape[1]
    tiles = out_ref.shape[0] // lanes // 2
    sub = lax.broadcasted_iota(I32, (lanes, lanes), 0)
    keys = keys_ref[...]
    upper = jnp.where(keys >= tiles * lanes, 1.0, 0.0).T
    middle = (keys >> 7) & (tiles - 1)
    low = []
    for chunk in range(chunks):
        low.append(jnp.where(sub == (keys[chunk : chunk + 1] & (lanes - 1)), 1.0, 0.0).astype(BF16))
        flag = jnp.broadcast_to(upper[:, chunk : chunk + 1], (lanes, columns)).astype(BF16)
        part = values_ref[chunk * lanes : (chunk + 1) * lanes, :]
        high_part = part * flag
        wide_ref[chunk * lanes : (chunk + 1) * lanes, :columns] = part - high_part
        wide_ref[chunk * lanes : (chunk + 1) * lanes, columns:] = high_part

    def tile_step(tile, carry):
        here = jnp.where(middle == tile, 1.0, 0.0)
        hot = [low[chunk] * jnp.broadcast_to(here[chunk : chunk + 1], (lanes, lanes)).astype(BF16) for chunk in range(chunks)]
        total = jnp.dot(jnp.concatenate(hot, axis=1), wide_ref[...], preferred_element_type=F32)
        out_ref[pl.ds(pl.multiple_of(tile * lanes, lanes), lanes), :] = total[:, :columns]
        out_ref[pl.ds(pl.multiple_of((tiles + tile) * lanes, lanes), lanes), :] = total[:, columns:]
        return carry

    lax.fori_loop(0, tiles, tile_step, 0)


def pack_last(sections, paired, early, late, scalar_ref, *refs):
    shared, (values_ref, keys_ref, groups_ref, dest_ref), refs = refs[:sections], refs[sections : sections + 4], refs[sections + 4 :]
    weights_ref, outs, (buffer_ref, meta_ref, kept_ref, count_ref) = refs[0], refs[1:-4], refs[-4:]
    owners = buffer_ref.shape[0]
    batches, blocks = dest_ref.shape
    rows = values_ref.shape[1]
    columns = weights_ref.shape[1]
    me, home = scalar_ref[sections], scalar_ref[sections + 1]
    count = batches * blocks
    own = pl.ds(pl.multiple_of(columns + home * count, count), count)
    kept = shared[0][own, :].astype(F32)
    for ref in shared[1:]:
        kept = kept * ref[own, :].astype(F32)
    kept_ref[...] = kept
    for k, ref in enumerate(shared):
        weights_ref[scalar_ref[k]] = ref[:columns, :]
    meta_ref[...] = jnp.zeros_like(meta_ref)
    meta_ref[:, :late, :] = jnp.full((owners, late, columns), -1.0, F32)
    buffer_ref[...] = jnp.zeros_like(buffer_ref)

    def visit(micro, block, owner, slot):
        at = owner ^ me if paired else owner
        meta_ref[at, pl.ds(FIELDS * late + slot, 1), :] = kept_ref[pl.ds(micro * blocks + block, 1), :]

        @pl.when(slot >= early)
        def _():
            lanes = pl.ds(pl.multiple_of(block * rows, rows), rows)
            source = (values_ref[micro * blocks + block], keys_ref[pl.ds(micro, 1), lanes], groups_ref[pl.ds(micro, 1), lanes])
            put_block(late, 0, source, at, slot - early, buffer_ref, meta_ref)

    walk_blocks(dest_ref, count_ref, owners, visit)
    buffer_ref[:, late * rows :, :] = meta_ref[...].astype(BF16)
    if len(outs) == 1:
        outs[0][...] = buffer_ref[...]
    else:
        for k, out in enumerate(outs):
            out[...] = buffer_ref[k]


def chain(values, weights):
    for weight in weights:
        half = jnp.dot(values, weight, preferred_element_type=F32) * 0.5
        values = (values.astype(F32) + (half + half * jnp.tanh(half))).astype(BF16)
    return values


def fetch_keys(meta_ref, start, slots, keys_ref, places_ref, sem):
    meta = meta_ref[:, start : start + 2 * slots, :].astype(F32)
    keys_ref[...] = (meta[:, :slots] * 128.0 + meta[:, slots:]).astype(I32)
    return pltpu.make_async_copy(keys_ref, places_ref, sem)


def find_rows(source, slots, at, rows, places_ref, table_ref, found_ref):
    for slot in range(slots):
        for row in range(rows):
            place = places_ref[source, slot, row]
            found_ref[pl.ds(at + slot * rows + row, 1), :] = table_ref[pl.ds(place, 1), :]


def join_first(slots, first_ref, weights_ref, table_ref, out_ref, keys_ref, found_ref, places_ref, sem):
    owners, columns = first_ref.shape[0], first_ref.shape[2]
    span = out_ref.shape[1]
    group = found_ref.shape[0] // span
    copy = fetch_keys(first_ref, span, slots, keys_ref, places_ref, sem)
    copy.start()
    weights = [weights_ref[j] for j in range(weights_ref.shape[0])]
    copy.wait()

    def step(turn, carry):
        base = turn * group
        values = first_ref[pl.ds(base, group), :span, :].reshape(group * span, columns)
        for source in range(group):
            find_rows(base + source, slots, source * span, span // slots, places_ref, table_ref, found_ref)
        joined = (chain(values, weights).astype(F32) * found_ref[...]).astype(BF16)
        out_ref[pl.ds(base, group)] = joined.reshape(group, span, columns)
        return carry

    lax.fori_loop(0, owners // group, step, 0)


def join_last(few, early, late, scalar_ref, first_ref, joined_ref, weights_ref, table_ref, *refs):
    parts, (out_ref, buffer_ref, meta_ref, keys_ref, found_ref, places_ref, list_ref, sem) = refs[:-8], refs[-8:]
    owners, span, columns = joined_ref.shape
    groups = out_ref.shape[0]
    rows = span // early
    batch = found_ref.shape[0] // rows
    me = scalar_ref[weights_ref.shape[0]]
    if few:
        for k, part in enumerate(parts):
            buffer_ref[me ^ k] = part[...]
    else:
        buffer_ref[...] = parts[0][...]
    copy = fetch_keys(buffer_ref, late * rows, late, keys_ref, places_ref, sem)
    copy.start()
    meta_ref[...] = buffer_ref[:, late * rows :, :].astype(F32)
    weights = [weights_ref[j] for j in range(weights_ref.shape[0])]
    sub = lax.broadcasted_iota(I32, (groups, rows), 0).astype(F32)
    step_size = math.gcd(owners, 8) if groups <= 128 else 1

    def early_step(turn, total):
        base = turn * step_size
        hot = []
        for source in range(step_size):
            meta = first_ref[base + source, span:, :].astype(F32)
            group = meta[2 * early : 3 * early] * 128.0 + meta[3 * early : 4 * early]
            group = jnp.where(meta_ref[base + source, FIELDS * late : FIELDS * late + early, :] > 0.5, group, -1.0)
            hot += [jnp.where(sub == group[j : j + 1], 1.0, 0.0).astype(BF16) for j in range(early)]
        joined = joined_ref[pl.ds(base, step_size)].reshape(step_size * span, columns)
        out_ref[...] += jnp.dot(jnp.concatenate(hot, axis=1), joined, preferred_element_type=F32)
        return total

    out_ref[...] = jnp.zeros_like(out_ref)
    lax.fori_loop(0, owners // step_size, early_step, 0)
    copy.wait()

    def note(source, count):
        for slot in range(late):
            list_ref[count] = source * late + slot
            count = count + jnp.where(places_ref[source, slot, 0] >= 0, 1, 0)
        return count

    filled = lax.fori_loop(0, owners, note, 0, unroll=min(owners, 8))

    def step(turn, carry):
        base = turn * batch
        values, hot = [], []
        for k in range(batch):
            there = base + k < filled
            item = list_ref[jnp.where(there, base + k, base)]
            source, slot = item // late, item % late
            values.append(buffer_ref[source, pl.ds(pl.multiple_of(slot * rows, rows), rows), :])
            group = meta_ref[source, pl.ds(2 * late + slot, 1), :] * 128.0 + meta_ref[source, pl.ds(3 * late + slot, 1), :]
            kept = meta_ref[source, pl.ds(FIELDS * late + early + slot, 1), :]
            group = jnp.where((kept > 0.5) & there, group, -1.0)
            hot.append(jnp.where(sub == group, 1.0, 0.0).astype(BF16))
            for row in range(rows):
                found_ref[k * rows + row : k * rows + row + 1, :] = table_ref[pl.ds(places_ref[source, slot, row], 1), :]
        joined = (chain(jnp.concatenate(values, axis=0), weights).astype(F32) * found_ref[...]).astype(BF16)
        out_ref[...] += jnp.dot(jnp.concatenate(hot, axis=1), joined, preferred_element_type=F32)
        return carry

    lax.fori_loop(0, (filled + batch - 1) // batch, step, 0)


def few_owners(owners):
    return owners <= 8 and owners & (owners - 1) == 0


def far_first(owners):
    return sorted(range(1, owners), key=lambda k: (-(k // (owners // 2)), -(k // 2), k))


def unpack_bits(bit_words):
    shifts = jnp.arange(16, dtype=jnp.int32)
    spread = jnp.right_shift(bit_words[..., None], shifts) & 1
    return spread.reshape(bit_words.shape[:-1] + (bit_words.shape[-1] * 16,))


def local(
    probe_values,
    probe_keys,
    group_ids,
    block_dest,
    filter_bits,
    section_weights,
    build_keys,
    build_values,
):
    sections = lax.axis_size("section")
    owners = lax.axis_size("owner")
    home = lax.axis_index("section").astype(I32)
    batches, block_count = block_dest.shape[:2]
    columns = probe_values.shape[2]
    rows = probe_values.shape[1] // block_count
    groups_all = GRP_DEV * sections * owners
    slots = batches * CAP
    late = slots // 2
    early = slots - late
    tile = 8
    early_meta = -(-FIELDS * early // tile) * tile
    late_meta = -(-(FIELDS * late + slots) // tile) * tile

    dest = block_dest.reshape(batches, block_count)
    blocks = probe_values.reshape(batches * block_count, rows, columns)
    counts = pltpu.SMEM((owners,), I32)
    first = run(
        functools.partial(pack_first, early),
        [dest, blocks, probe_keys, group_ids],
        ((owners, early * rows + early_meta, columns), BF16),
        [
            pltpu.SMEM(dest.shape, I32),
            pltpu.VMEM(blocks.shape, BF16),
            pltpu.VMEM(probe_keys.shape, I32),
            pltpu.VMEM(group_ids.shape, I32),
            pltpu.VMEM((owners, early_meta, columns), F32),
            counts,
            pltpu.SemaphoreType.DMA((4,)),
        ],
        away=True,
    )
    first = lax.all_to_all(first, "owner", split_axis=0, concat_axis=0, tiled=True)

    bits = unpack_bits(filter_bits[0]).astype(BF16).reshape(-1, rows)
    shared = jnp.concatenate([section_weights[0], bits], axis=0)
    paired = sections & (sections - 1) == 0

    def partner(index, k):
        return index ^ k if paired else (index - k) % sections

    received = [shared] + [
        lax.ppermute(shared, "section", [(partner(i, k), i) for i in range(sections)]) for k in range(1, sections)
    ]
    scalars = jnp.stack(
        [lax.rem(partner(home, k) - home + sections, sections) for k in range(sections)]
        + [lax.axis_index("owner").astype(I32), home]
    )
    table = run(
        build_table,
        [build_keys.reshape(-1, 128), build_values],
        ((KEYS_OWN, columns), F32),
        [pltpu.VMEM((build_values.shape[0], 2 * columns), BF16)],
        flops=2 * KEYS_OWN * build_keys.shape[0] * columns,
    )
    few = few_owners(owners)
    part = (late * rows + late_meta, columns)
    weights, *parts = run(
        functools.partial(pack_last, sections, few, early, late),
        [scalars] + received + [blocks, probe_keys, group_ids, dest],
        [((sections, columns, columns), BF16)] + ([(part, BF16)] * owners if few else [((owners, *part), BF16)]),
        [
            pltpu.VMEM((owners, *part), BF16),
            pltpu.VMEM((owners, late_meta, columns), F32),
            pltpu.VMEM((batches * block_count, rows), F32),
            counts,
        ],
        scalars=(0, 1 + sections + 3),
    )
    if few:
        for k in far_first(owners):
            parts[k] = lax.ppermute(parts[k], "owner", [(i, i ^ k) for i in range(owners)])
    else:
        parts = [lax.all_to_all(parts[0], "owner", split_axis=0, concat_axis=0, tiled=True)]

    group = math.gcd(owners, 4)
    joined = run(
        functools.partial(join_first, early),
        [first, weights, table],
        ((owners, early * rows, columns), BF16),
        [
            pltpu.VMEM((owners, early, rows), I32),
            pltpu.VMEM((group * early * rows, columns), F32),
            pltpu.SMEM((owners, early, rows), I32),
            pltpu.SemaphoreType.DMA,
        ],
        flops=2 * KEYS_OWN * owners * early * rows * columns,
    )
    sums = run(
        functools.partial(join_last, few, early, late),
        [scalars, first, joined, weights, table] + parts,
        ((groups_all, columns), F32),
        [
            pltpu.VMEM((owners, *part), BF16),
            pltpu.VMEM((owners, late_meta, columns), F32),
            pltpu.VMEM((owners, late, rows), I32),
            pltpu.VMEM((4 * rows, columns), F32),
            pltpu.SMEM((owners, late, rows), I32),
            pltpu.SMEM((owners * late + 1,), I32),
            pltpu.SemaphoreType.DMA,
        ],
        scalars=(0,),
        flops=2 * groups_all * owners * slots * rows * columns,
    )
    parts = sums.reshape(sections * owners, GRP_DEV, columns)
    parts = lax.all_to_all(parts, ("section", "owner"), split_axis=0, concat_axis=0, tiled=True)
    return jnp.sum(parts, axis=0)


def solution(mesh):
    placed = (
        P("section", "owner", None),
        P("section", "owner"),
        P("section", "owner"),
        P("section", "owner", None),
        P("section", None, "owner"),
        P("section", None, None),
        P("owner"),
        P("owner", None),
    )
    return jax.shard_map(
        local, mesh=mesh, in_specs=placed, out_specs=P(("section", "owner"), None), check_vma=False
    )
```

```python
import functools
import math

import jax
import jax.numpy as jnp
from jax import lax
from jax.experimental import pallas as pl
from jax.experimental.pallas import tpu as pltpu
from jax.sharding import PartitionSpec as P


CAP = 2
KEYS_OWN = 2048
GRP_DEV = 4
FIELDS = 3
MASKED = -16384.0
BF16 = jnp.bfloat16
F32 = jnp.float32
I32 = jnp.int32


def run(kernel, ins, outs, scratch=(), scalars=(), flops=0, away=False):
    several = isinstance(outs, list)
    shapes = [jax.ShapeDtypeStruct(shape, dtype) for shape, dtype in (outs if several else [outs])]
    held = shapes + [x for k, x in enumerate(ins) if k not in scalars and not away]
    size = sum(math.prod(x.shape) * x.dtype.itemsize for x in held)
    for entry in scratch:
        size += 2 * math.prod(getattr(entry, "shape", ())) * 4
    place = pl.BlockSpec(memory_space=pltpu.VMEM)
    spaces = [pltpu.HBM if away else pltpu.SMEM if k in scalars else pltpu.VMEM for k in range(len(ins))]
    return pl.pallas_call(
        kernel,
        out_shape=shapes if several else shapes[0],
        in_specs=[pl.BlockSpec(memory_space=space) for space in spaces],
        out_specs=[place] * len(shapes) if several else place,
        scratch_shapes=list(scratch),
        compiler_params=pltpu.CompilerParams(vmem_limit_bytes=60 * 2**20 if away else min(size + 4 * 2**20, 60 * 2**20)),
        cost_estimate=pl.CostEstimate(flops=flops, bytes_accessed=size, transcendentals=0) if flops else None,
    )(*ins)


def walk_blocks(dest_ref, count_ref, owners, visit):
    batches, blocks = dest_ref.shape

    def clear(owner, carry):
        count_ref[owner] = 0
        return carry

    lax.fori_loop(0, owners, clear, 0)
    for micro in range(batches):

        def step(block, carry, micro=micro):
            owner = dest_ref[micro, block]
            slot = count_ref[owner]
            count_ref[owner] = slot + 1
            visit(micro, block, owner, slot)
            return carry

        lax.fori_loop(0, blocks, step, 0, unroll=min(blocks, 8))


def put_block(slots, source, kept, owner_at, slot, out_ref, meta_ref):
    values, keys, groups = source
    rows = values.shape[0]
    out_ref[owner_at, pl.ds(pl.multiple_of(slot * rows, rows), rows), :] = values
    high = ((groups >> 7) * (KEYS_OWN // 128) + (keys >> 7)).astype(F32)
    low = (groups & 127).astype(F32)
    if kept is not None:
        low = jnp.where(kept > 0.5, low, MASKED)
    for field, part in enumerate((high, (keys & 127).astype(F32), low)):
        meta_ref[owner_at, pl.ds(field * slots + slot, 1), :] = part


def key_of(high, low):
    return (high.astype(I32) & (KEYS_OWN // 128 - 1)) * 128 + low.astype(I32)


def group_of(high, low):
    return (high.astype(I32) // (KEYS_OWN // 128) * 128).astype(F32) + low


def share_bits(words_ref, weight_ref, shared_ref):
    columns = weight_ref.shape[0]
    shared_ref[:columns, :] = weight_ref[...]
    words = words_ref[...]
    micros, length = words.shape
    parts = jnp.concatenate([words & 255, words >> 8], axis=0).astype(F32).astype(BF16)
    width = min(length, 128)
    spread = lax.broadcasted_iota(I32, (width, width * 16), 1) // 16 == lax.broadcasted_iota(I32, (width, width * 16), 0)
    spread = jnp.where(spread, 1.0, 0.0).astype(BF16)
    place = lax.broadcasted_iota(I32, (micros, width * 16), 1) & 15
    for turn in range(length // width):
        found = jnp.dot(parts[:, turn * width : (turn + 1) * width], spread, preferred_element_type=F32).astype(I32)
        bits = (jnp.where(place < 8, found[:micros], found[micros:]) >> (place & 7)) & 1
        stacked = jnp.concatenate([bits[:, k : k + 128] for k in range(0, width * 16, 128)], axis=0)
        start = columns + turn * stacked.shape[0]
        shared_ref[start : start + stacked.shape[0], :] = stacked.astype(F32).astype(BF16)


def pack_first(early, *refs):
    sources, (out_ref, shared_ref), held, (meta_ref, count_ref, sems) = refs[:6], refs[6:8], refs[8:14], refs[14:]
    dest_ref, values_ref, keys_ref, groups_ref, words_ref, weight_ref = held
    owners = out_ref.shape[0]
    blocks = dest_ref.shape[1]
    rows = values_ref.shape[1]
    copies = [pltpu.make_async_copy(source, target, sems.at[k]) for k, (source, target) in enumerate(zip(sources, held))]
    for copy in copies:
        copy.start()
    meta_ref[...] = jnp.zeros_like(meta_ref)
    out_ref[...] = jnp.zeros_like(out_ref)
    copies[4].wait()
    copies[5].wait()
    share_bits(words_ref, weight_ref, shared_ref)
    for copy in copies[:4]:
        copy.wait()

    def visit(micro, block, owner, slot):
        @pl.when(slot < early)
        def _():
            lanes = pl.ds(pl.multiple_of(block * rows, rows), rows)
            source = (values_ref[micro * blocks + block], keys_ref[pl.ds(micro, 1), lanes], groups_ref[pl.ds(micro, 1), lanes])
            put_block(early, source, None, owner, slot, out_ref, meta_ref)

    walk_blocks(dest_ref, count_ref, owners, visit)
    out_ref[:, early * rows :, :] = meta_ref[...].astype(BF16)


def build_table(keys_ref, values_ref, out_ref, wide_ref):
    chunks, lanes = keys_ref.shape
    columns = values_ref.shape[1]
    tiles = out_ref.shape[0] // lanes // 2
    sub = lax.broadcasted_iota(I32, (lanes, lanes), 0)
    keys = keys_ref[...]
    upper = jnp.where(keys >= tiles * lanes, 1.0, 0.0).T
    middle = (keys >> 7) & (tiles - 1)
    low = []
    for chunk in range(chunks):
        low.append(jnp.where(sub == (keys[chunk : chunk + 1] & (lanes - 1)), 1.0, 0.0).astype(BF16))
        flag = jnp.broadcast_to(upper[:, chunk : chunk + 1], (lanes, columns)).astype(BF16)
        part = values_ref[chunk * lanes : (chunk + 1) * lanes, :]
        high_part = part * flag
        wide_ref[chunk * lanes : (chunk + 1) * lanes, :columns] = part - high_part
        wide_ref[chunk * lanes : (chunk + 1) * lanes, columns:] = high_part

    def tile_step(tile, carry):
        here = jnp.where(middle == tile, 1.0, 0.0)
        hot = [low[chunk] * jnp.broadcast_to(here[chunk : chunk + 1], (lanes, lanes)).astype(BF16) for chunk in range(chunks)]
        total = jnp.dot(jnp.concatenate(hot, axis=1), wide_ref[...], preferred_element_type=F32)
        out_ref[pl.ds(pl.multiple_of(tile * lanes, lanes), lanes), :] = total[:, :columns]
        out_ref[pl.ds(pl.multiple_of((tiles + tile) * lanes, lanes), lanes), :] = total[:, columns:]
        return carry

    lax.fori_loop(0, tiles, tile_step, 0)


def pack_last(sections, paired, early, late, scalar_ref, *refs):
    shared, (values_ref, keys_ref, groups_ref, dest_ref), refs = refs[:sections], refs[sections : sections + 4], refs[sections + 4 :]
    weights_ref, outs, (buffer_ref, meta_ref, kept_ref, count_ref) = refs[0], refs[1:-4], refs[-4:]
    owners = buffer_ref.shape[0]
    batches, blocks = dest_ref.shape
    rows = values_ref.shape[1]
    columns = weights_ref.shape[1]
    me, home = scalar_ref[sections], scalar_ref[sections + 1]
    kept = shared[0][columns:, :].astype(F32)
    for ref in shared[1:]:
        kept = kept * ref[columns:, :].astype(F32)
    kept_ref[...] = kept
    micros = kept.shape[0] // blocks
    for k, ref in enumerate(shared):
        weights_ref[scalar_ref[k]] = (ref[:columns, :].astype(F32) * 0.5).astype(BF16)
    meta_ref[...] = jnp.zeros_like(meta_ref)
    buffer_ref[...] = jnp.zeros_like(buffer_ref)

    def visit(micro, block, owner, slot):
        at = owner ^ me if paired else owner
        kept = kept_ref[pl.ds(block * micros + home * batches + micro, 1), :]

        @pl.when(slot < early)
        def _():
            meta_ref[at, pl.ds(FIELDS * late + slot, 1), :] = kept

        @pl.when(slot >= early)
        def _():
            lanes = pl.ds(pl.multiple_of(block * rows, rows), rows)
            source = (values_ref[micro * blocks + block], keys_ref[pl.ds(micro, 1), lanes], groups_ref[pl.ds(micro, 1), lanes])
            put_block(late, source, kept, at, slot - early, buffer_ref, meta_ref)

    walk_blocks(dest_ref, count_ref, owners, visit)
    buffer_ref[:, late * rows :, :] = meta_ref[...].astype(BF16)
    if len(outs) == 1:
        outs[0][...] = buffer_ref[...]
    else:
        for k, out in enumerate(outs):
            out[...] = buffer_ref[k]


def chain(values, weights):
    for weight in weights:
        half = jnp.dot(values, weight, preferred_element_type=F32)
        values = (values.astype(F32) + (half + half * jnp.tanh(half))).astype(BF16)
    return values


def join_rows(values, weights, rows, place_of, table_ref, found_ref):
    count = values.shape[0] // rows
    for block in range(count):
        for row in range(rows):
            found_ref[block * rows + row : block * rows + row + 1, :] = table_ref[pl.ds(place_of(block, row), 1), :]
    return (chain(values, weights).astype(F32) * found_ref[...]).astype(BF16)


def over(count, stride, step):
    if count <= 8:
        for base in range(0, count, stride):
            step(base)
    else:

        def turn(k, carry):
            step(k * stride)
            return carry

        lax.fori_loop(0, count // stride, turn, 0)


def join_first(slots, first_ref, weights_ref, table_ref, out_ref, keys_ref, found_ref, places_ref, sem):
    owners, columns = first_ref.shape[0], first_ref.shape[2]
    span = out_ref.shape[1]
    rows = span // slots
    group = found_ref.shape[0] // span
    meta = first_ref[:, span:, :].astype(F32)
    keys_ref[...] = key_of(meta[:, :slots], meta[:, slots : 2 * slots])
    copy = pltpu.make_async_copy(keys_ref, places_ref, sem)
    copy.start()
    weights = [weights_ref[j] for j in range(weights_ref.shape[0])]
    copy.wait()

    def step(base):
        values = first_ref[pl.ds(base, group), :span, :].reshape(group * span, columns)
        joined = join_rows(
            values,
            weights,
            rows,
            lambda block, row: places_ref[base + block // slots, block % slots, row],
            table_ref,
            found_ref,
        )
        out_ref[pl.ds(base, group)] = joined.reshape(group, span, columns)

    over(owners, group, step)


def join_last(few, early, late, scalar_ref, first_ref, joined_ref, weights_ref, table_ref, *refs):
    parts, (out_ref, keys_ref, found_ref, places_ref, sem) = refs[:-5], refs[-5:]
    owners, span, _ = joined_ref.shape
    groups = out_ref.shape[0]
    rows = span // early
    late_span = late * rows
    group = found_ref.shape[0] // late_span
    me = scalar_ref[weights_ref.shape[0]]

    def part_of(k):
        return parts[k] if few else parts[0].at[k]

    if few:
        for k, part in enumerate(parts):
            meta = part[late_span:, :].astype(F32)
            keys_ref[k] = key_of(meta[:late], meta[late : 2 * late])
    else:
        meta = parts[0][:, late_span:, :].astype(F32)
        keys_ref[...] = key_of(meta[:, :late], meta[:, late : 2 * late])
    copy = pltpu.make_async_copy(keys_ref, places_ref, sem)
    copy.start()
    weights = [weights_ref[j] for j in range(weights_ref.shape[0])]
    sub = lax.broadcasted_iota(I32, (groups, rows), 0).astype(F32)

    def hot_rows(group_keys):
        return [jnp.where(sub == group_keys[j : j + 1], 1.0, 0.0).astype(BF16) for j in range(group_keys.shape[0])]

    out_ref[...] = jnp.zeros_like(out_ref)

    def early_step(base):
        hot, joined = [], []
        for k in range(group):
            source = me ^ (base + k) if few else base + k
            meta = first_ref[source, span:, :].astype(F32)
            kept = part_of(base + k)[late_span:, :].astype(F32)[FIELDS * late : FIELDS * late + early]
            keys = group_of(meta[:early], meta[2 * early : 3 * early])
            hot += hot_rows(jnp.where(kept > 0.5, keys, -1.0))
            joined.append(joined_ref[source])
        out_ref[...] += jnp.dot(
            jnp.concatenate(hot, axis=1), jnp.concatenate(joined, axis=0), preferred_element_type=F32
        )

    over(owners, group, early_step)
    copy.wait()

    def step(base):
        values = jnp.concatenate([part_of(base + k)[:late_span, :] for k in range(group)], axis=0)
        hot = []
        for k in range(group):
            meta = part_of(base + k)[late_span:, :].astype(F32)
            hot += hot_rows(group_of(meta[:late], meta[2 * late : 3 * late]))
        joined = join_rows(
            values,
            weights,
            rows,
            lambda block, row: places_ref[base + block // late, block % late, row],
            table_ref,
            found_ref,
        )
        out_ref[...] += jnp.dot(jnp.concatenate(hot, axis=1), joined, preferred_element_type=F32)

    over(owners, group, step)


def few_owners(owners):
    return owners <= 8 and owners & (owners - 1) == 0


def far_first(owners):
    return sorted(range(1, owners), key=lambda k: (-(k // (owners // 2)), -(k // 2), k))


def local(
    probe_values,
    probe_keys,
    group_ids,
    block_dest,
    filter_bits,
    section_weights,
    build_keys,
    build_values,
):
    sections = lax.axis_size("section")
    owners = lax.axis_size("owner")
    home = lax.axis_index("section").astype(I32)
    batches, block_count = block_dest.shape[:2]
    columns = probe_values.shape[2]
    rows = probe_values.shape[1] // block_count
    groups_all = GRP_DEV * sections * owners
    slots = batches * CAP
    late = slots // 2
    early = slots - late
    tile = 8
    early_meta = -(-FIELDS * early // tile) * tile
    late_meta = -(-(FIELDS * late + early) // tile) * tile

    dest = block_dest.reshape(batches, block_count)
    blocks = probe_values.reshape(batches * block_count, rows, columns)
    counts = pltpu.SMEM((owners,), I32)
    words = filter_bits[0]
    micros = words.shape[0]
    shared_shape = (columns + micros * block_count, columns)
    sources = [dest, blocks, probe_keys, group_ids, words, section_weights[0]]
    first, shared = run(
        functools.partial(pack_first, early),
        sources,
        [((owners, early * rows + early_meta, columns), BF16), (shared_shape, BF16)],
        [pltpu.SMEM(dest.shape, I32)]
        + [pltpu.VMEM(source.shape, source.dtype) for source in sources[1:]]
        + [pltpu.VMEM((owners, early_meta, columns), F32), counts, pltpu.SemaphoreType.DMA((len(sources),))],
        away=True,
    )
    first = lax.all_to_all(first, "owner", split_axis=0, concat_axis=0, tiled=True)

    paired = sections & (sections - 1) == 0

    def partner(index, k):
        return index ^ k if paired else (index - k) % sections

    received = [shared] + [
        lax.ppermute(shared, "section", [(partner(i, k), i) for i in range(sections)]) for k in range(1, sections)
    ]
    scalars = jnp.stack(
        [lax.rem(partner(home, k) - home + sections, sections) for k in range(sections)]
        + [lax.axis_index("owner").astype(I32), home]
    )
    table = run(
        build_table,
        [build_keys.reshape(-1, 128), build_values],
        ((KEYS_OWN, columns), F32),
        [pltpu.VMEM((build_values.shape[0], 2 * columns), BF16)],
        flops=2 * KEYS_OWN * build_keys.shape[0] * columns,
    )
    few = few_owners(owners)
    part = (late * rows + late_meta, columns)
    weights, *parts = run(
        functools.partial(pack_last, sections, few, early, late),
        [scalars] + received + [blocks, probe_keys, group_ids, dest],
        [((sections, columns, columns), BF16)] + ([(part, BF16)] * owners if few else [((owners, *part), BF16)]),
        [
            pltpu.VMEM((owners, *part), BF16),
            pltpu.VMEM((owners, late_meta, columns), F32),
            pltpu.VMEM((micros * block_count, rows), F32),
            counts,
        ],
        scalars=(0, 1 + sections + 3),
    )
    if few:
        for k in far_first(owners):
            parts[k] = lax.ppermute(parts[k], "owner", [(i, i ^ k) for i in range(owners)])
    else:
        parts = [lax.all_to_all(parts[0], "owner", split_axis=0, concat_axis=0, tiled=True)]

    group = math.gcd(owners, 4)
    joined = run(
        functools.partial(join_first, early),
        [first, weights, table],
        ((owners, early * rows, columns), BF16),
        [
            pltpu.VMEM((owners, early, rows), I32),
            pltpu.VMEM((group * early * rows, columns), F32),
            pltpu.SMEM((owners, early, rows), I32),
            pltpu.SemaphoreType.DMA,
        ],
        flops=2 * KEYS_OWN * owners * early * rows * columns,
    )
    sums = run(
        functools.partial(join_last, few, early, late),
        [scalars, first, joined, weights, table] + parts,
        ((groups_all, columns), F32),
        [
            pltpu.VMEM((owners, late, rows), I32),
            pltpu.VMEM((group * late * rows, columns), F32),
            pltpu.SMEM((owners, late, rows), I32),
            pltpu.SemaphoreType.DMA,
        ],
        scalars=(0,),
        flops=2 * groups_all * owners * slots * rows * columns,
    )
    parts = sums.reshape(sections * owners, GRP_DEV, columns)
    parts = lax.all_to_all(parts, ("section", "owner"), split_axis=0, concat_axis=0, tiled=True)
    return jnp.sum(parts, axis=0)


def solution(mesh):
    placed = (
        P("section", "owner", None),
        P("section", "owner"),
        P("section", "owner"),
        P("section", "owner", None),
        P("section", None, "owner"),
        P("section", None, None),
        P("owner"),
        P("owner", None),
    )
    return jax.shard_map(
        local, mesh=mesh, in_specs=placed, out_specs=P(("section", "owner"), None), check_vma=False
    )
```

```python
import functools
import math

import jax
import jax.numpy as jnp
from jax import lax
from jax.experimental import pallas as pl
from jax.experimental.pallas import tpu as pltpu
from jax.sharding import PartitionSpec as P


CAP = 2
KEYS_OWN = 2048
GRP_DEV = 4
FIELDS = 3
BF16 = jnp.bfloat16
F32 = jnp.float32
I32 = jnp.int32


def run(kernel, ins, outs, scratch=(), scalars=(), flops=0, away=False):
    several = isinstance(outs, list)
    shapes = [jax.ShapeDtypeStruct(shape, dtype) for shape, dtype in (outs if several else [outs])]
    held = shapes + [x for k, x in enumerate(ins) if k not in scalars and not away]
    size = sum(math.prod(x.shape) * x.dtype.itemsize for x in held)
    for entry in scratch:
        size += 2 * math.prod(getattr(entry, "shape", ())) * 4
    place = pl.BlockSpec(memory_space=pltpu.VMEM)
    spaces = [pltpu.SMEM if k in scalars else pltpu.HBM if away else pltpu.VMEM for k in range(len(ins))]
    return pl.pallas_call(
        kernel,
        out_shape=shapes if several else shapes[0],
        in_specs=[pl.BlockSpec(memory_space=space) for space in spaces],
        out_specs=[place] * len(shapes) if several else place,
        scratch_shapes=list(scratch),
        compiler_params=pltpu.CompilerParams(vmem_limit_bytes=60 * 2**20 if away else min(size + 4 * 2**20, 60 * 2**20)),
        cost_estimate=pl.CostEstimate(flops=flops, bytes_accessed=size, transcendentals=0) if flops else None,
    )(*ins)


def walk_blocks(dest_ref, count_ref, owners, visit):
    batches, blocks = dest_ref.shape

    def clear(owner, carry):
        count_ref[owner] = 0
        return carry

    lax.fori_loop(0, owners, clear, 0)
    for micro in range(batches):

        def step(block, carry, micro=micro):
            owner = dest_ref[micro, block]
            slot = count_ref[owner]
            count_ref[owner] = slot + 1
            visit(micro, block, owner, slot)
            return carry

        lax.fori_loop(0, blocks, step, 0, unroll=min(blocks, 8))


def put_block(slots, source, owner_at, slot, out_ref, meta_ref):
    values, keys, groups = source
    rows = values.shape[0]
    out_ref[owner_at, pl.ds(pl.multiple_of(slot * rows, rows), rows), :] = values
    high = ((groups >> 7) * (KEYS_OWN // 128) + (keys >> 7)).astype(F32)
    low = (groups & 127).astype(F32)
    for field, part in enumerate((high, (keys & 127).astype(F32), low)):
        meta_ref[owner_at, pl.ds(field * slots + slot, 1), :] = part


def key_of(high, low):
    return (high.astype(I32) & (KEYS_OWN // 128 - 1)) * 128 + low.astype(I32)


def group_of(high, low):
    return (high.astype(I32) // (KEYS_OWN // 128) * 128).astype(F32) + low


def share_bits(words_ref, weight_ref, shared_ref):
    columns = weight_ref.shape[0]
    shared_ref[:columns, :] = weight_ref[...]
    words = words_ref[...]
    micros, length = words.shape
    parts = jnp.concatenate([words & 255, words >> 8], axis=0).astype(F32).astype(BF16)
    width = min(length, 128)
    spread = lax.broadcasted_iota(I32, (width, width * 16), 1) // 16 == lax.broadcasted_iota(I32, (width, width * 16), 0)
    spread = jnp.where(spread, 1.0, 0.0).astype(BF16)
    place = lax.broadcasted_iota(I32, (micros, width * 16), 1) & 15
    for turn in range(length // width):
        found = jnp.dot(parts[:, turn * width : (turn + 1) * width], spread, preferred_element_type=F32).astype(I32)
        bits = (jnp.where(place < 8, found[:micros], found[micros:]) >> (place & 7)) & 1
        stacked = jnp.concatenate([bits[:, k : k + 128] for k in range(0, width * 16, 128)], axis=0)
        start = columns + turn * stacked.shape[0]
        shared_ref[start : start + stacked.shape[0], :] = stacked.astype(F32).astype(BF16)


def pack_first(few, slots, me_ref, *refs):
    sources, shared_ref, outs, held = refs[:6], refs[6], refs[7:-10], refs[-10:-4]
    buffer_ref, meta_ref, count_ref, sems = refs[-4:]
    dest_ref, values_ref, keys_ref, groups_ref, words_ref, weight_ref = held
    owners = buffer_ref.shape[0]
    blocks = dest_ref.shape[1]
    rows = values_ref.shape[1]
    copies = [pltpu.make_async_copy(source, target, sems.at[k]) for k, (source, target) in enumerate(zip(sources, held))]
    for copy in copies:
        copy.start()
    meta_ref[...] = jnp.zeros_like(meta_ref)
    buffer_ref[...] = jnp.zeros_like(buffer_ref)
    me = me_ref[0]
    copies[4].wait()
    copies[5].wait()
    share_bits(words_ref, weight_ref, shared_ref)
    for copy in copies[:4]:
        copy.wait()

    def visit(micro, block, owner, slot):
        lanes = pl.ds(pl.multiple_of(block * rows, rows), rows)
        source = (values_ref[micro * blocks + block], keys_ref[pl.ds(micro, 1), lanes], groups_ref[pl.ds(micro, 1), lanes])
        put_block(slots, source, owner ^ me if few else owner, slot, buffer_ref, meta_ref)

    walk_blocks(dest_ref, count_ref, owners, visit)
    buffer_ref[:, slots * rows :, :] = meta_ref[...].astype(BF16)
    if few:
        for k, out in enumerate(outs):
            out[...] = buffer_ref[k]
    else:
        outs[0][...] = buffer_ref[...]


def build_table(keys_ref, values_ref, out_ref, wide_ref):
    chunks, lanes = keys_ref.shape
    columns = values_ref.shape[1]
    tiles = out_ref.shape[0] // lanes // 2
    sub = lax.broadcasted_iota(I32, (lanes, lanes), 0)
    keys = keys_ref[...]
    upper = jnp.where(keys >= tiles * lanes, 1.0, 0.0).T
    middle = (keys >> 7) & (tiles - 1)
    low = []
    for chunk in range(chunks):
        low.append(jnp.where(sub == (keys[chunk : chunk + 1] & (lanes - 1)), 1.0, 0.0).astype(BF16))
        flag = jnp.broadcast_to(upper[:, chunk : chunk + 1], (lanes, columns)).astype(BF16)
        part = values_ref[chunk * lanes : (chunk + 1) * lanes, :]
        high_part = part * flag
        wide_ref[chunk * lanes : (chunk + 1) * lanes, :columns] = part - high_part
        wide_ref[chunk * lanes : (chunk + 1) * lanes, columns:] = high_part

    def tile_step(tile, carry):
        here = jnp.where(middle == tile, 1.0, 0.0)
        hot = [low[chunk] * jnp.broadcast_to(here[chunk : chunk + 1], (lanes, lanes)).astype(BF16) for chunk in range(chunks)]
        total = jnp.dot(jnp.concatenate(hot, axis=1), wide_ref[...], preferred_element_type=F32)
        out_ref[pl.ds(pl.multiple_of(tile * lanes, lanes), lanes), :] = total[:, :columns]
        out_ref[pl.ds(pl.multiple_of((tiles + tile) * lanes, lanes), lanes), :] = total[:, columns:]
        return carry

    lax.fori_loop(0, tiles, tile_step, 0)


def place_bits(sections, scalar_ref, *refs):
    shared, (dest_ref, weights_ref, out_ref, kept_ref, count_ref) = refs[:sections], refs[sections:]
    owners = out_ref.shape[0]
    batches, blocks = dest_ref.shape
    columns = weights_ref.shape[1]
    home = scalar_ref[sections + 1]
    kept = shared[0][columns:, :].astype(F32)
    for ref in shared[1:]:
        kept = kept * ref[columns:, :].astype(F32)
    kept_ref[...] = kept
    micros = kept.shape[0] // blocks
    for k, ref in enumerate(shared):
        weights_ref[scalar_ref[k]] = (ref[:columns, :].astype(F32) * 0.5).astype(BF16)
    out_ref[...] = jnp.zeros_like(out_ref)

    def visit(micro, block, owner, slot):
        out_ref[owner, pl.ds(slot, 1), :] = kept_ref[pl.ds(block * micros + home * batches + micro, 1), :]

    walk_blocks(dest_ref, count_ref, owners, visit)


def chain(values, weights):
    for weight in weights:
        half = jnp.dot(values, weight, preferred_element_type=F32)
        values = (values.astype(F32) + (half + half * jnp.tanh(half))).astype(BF16)
    return values


def join_rows(values, weights, rows, place_of, table_ref, found_ref):
    count = values.shape[0] // rows
    for block in range(count):
        for row in range(rows):
            found_ref[block * rows + row : block * rows + row + 1, :] = table_ref[pl.ds(place_of(block, row), 1), :]
    return (chain(values, weights).astype(F32) * found_ref[...]).astype(BF16)


def start_keys(parts, slots, span, keys_ref, places_ref, sem):
    for k, part in enumerate(parts):
        meta = part[span:, :].astype(F32)
        keys_ref[k] = key_of(meta[:slots], meta[slots : 2 * slots])
    copy = pltpu.make_async_copy(keys_ref, places_ref, sem)
    copy.start()
    return copy


def join_parts(parts, first, slots, span, weights, table_ref, found_ref, places_ref):
    values = jnp.concatenate([part[:span, :] for part in parts], axis=0)
    return join_rows(
        values,
        weights,
        span // slots,
        lambda block, row: places_ref[first + block // slots, block % slots, row],
        table_ref,
        found_ref,
    )


def sums_of(parts, kepts, joined, slots, span, groups):
    sub = lax.broadcasted_iota(I32, (groups, span // slots), 0).astype(F32)
    hot = []
    for part, kept in zip(parts, kepts):
        meta = part[span:, :].astype(F32)
        keys = group_of(meta[:slots], meta[2 * slots : 3 * slots])
        keys = jnp.where(kept[:slots] > 0.5, keys, -1.0)
        hot += [jnp.where(sub == keys[j : j + 1], 1.0, 0.0).astype(BF16) for j in range(slots)]
    return jnp.dot(jnp.concatenate(hot, axis=1), joined, preferred_element_type=F32)


def join_only(slots, weights_ref, table_ref, *refs):
    parts, (out_ref, keys_ref, found_ref, places_ref, sem) = refs[:-5], refs[-5:]
    span = out_ref.shape[1]
    group = found_ref.shape[0] // span
    copy = start_keys(parts, slots, span, keys_ref, places_ref, sem)
    weights = [weights_ref[j] for j in range(weights_ref.shape[0])]
    copy.wait()
    for at in range(0, len(parts), group):
        joined = join_parts(parts[at : at + group], at, slots, span, weights, table_ref, found_ref, places_ref)
        out_ref[at : at + group] = joined.reshape(group, span, joined.shape[1])


def join_sum(slots, span, new, old, carried, scalar_ref, kept_ref, weights_ref, table_ref, *refs):
    news, olds, refs = refs[: len(new)], refs[len(new) : len(new) + len(old)], refs[len(new) + len(old) :]
    before, (out_ref, keys_ref, found_ref, places_ref, sem) = refs[:-5], refs[-5:]
    groups = out_ref.shape[0]
    group = found_ref.shape[0] // span
    me = scalar_ref[weights_ref.shape[0]]
    copy = start_keys(news, slots, span, keys_ref, places_ref, sem)
    weights = [weights_ref[j] for j in range(weights_ref.shape[0])]
    total = before[-1][...] if carried else jnp.zeros(out_ref.shape, F32)
    if old:
        joined = before[0][...].reshape(len(old) * span, out_ref.shape[1])
        total += sums_of(olds, [kept_ref[me ^ k] for k in old], joined, slots, span, groups)
    copy.wait()
    for at in range(0, len(new), group):
        these = news[at : at + group]
        joined = join_parts(these, at, slots, span, weights, table_ref, found_ref, places_ref)
        total += sums_of(these, [kept_ref[me ^ k] for k in new[at : at + group]], joined, slots, span, groups)
    out_ref[...] = total


def join_all(slots, span, kept_ref, weights_ref, table_ref, first_ref, out_ref, keys_ref, found_ref, places_ref, sem):
    groups = out_ref.shape[0]
    meta = first_ref[:, span:, :].astype(F32)
    keys_ref[...] = key_of(meta[:, :slots], meta[:, slots : 2 * slots])
    copy = pltpu.make_async_copy(keys_ref, places_ref, sem)
    copy.start()
    weights = [weights_ref[j] for j in range(weights_ref.shape[0])]
    out_ref[...] = jnp.zeros_like(out_ref)
    copy.wait()

    def step(source, carry):
        part = first_ref.at[source]
        joined = join_parts([part], source, slots, span, weights, table_ref, found_ref, places_ref)
        out_ref[...] += sums_of([part], [kept_ref[source]], joined, slots, span, groups)
        return carry

    lax.fori_loop(0, first_ref.shape[0], step, 0)


def few_owners(owners):
    return 4 < owners <= 8 and owners & (owners - 1) == 0


def far_first(owners):
    return sorted(range(1, owners), key=lambda k: -(k // 2) * owners + k)


def local(
    probe_values,
    probe_keys,
    group_ids,
    block_dest,
    filter_bits,
    section_weights,
    build_keys,
    build_values,
):
    sections = lax.axis_size("section")
    owners = lax.axis_size("owner")
    home = lax.axis_index("section").astype(I32)
    batches, block_count = block_dest.shape[:2]
    columns = probe_values.shape[2]
    rows = probe_values.shape[1] // block_count
    groups_all = GRP_DEV * sections * owners
    slots = batches * CAP
    span = slots * rows
    height = span + -(-FIELDS * slots // 8) * 8
    few = few_owners(owners)
    paired = sections & (sections - 1) == 0

    def partner(index, k):
        return index ^ k if paired else (index - k) % sections

    me = lax.axis_index("owner").astype(I32)
    scalars = jnp.stack([lax.rem(partner(home, k) - home + sections, sections) for k in range(sections)] + [me, home])
    dest = block_dest.reshape(batches, block_count)
    blocks = probe_values.reshape(batches * block_count, rows, columns)
    words = filter_bits[0]
    micros = words.shape[0]
    counts = pltpu.SMEM((owners,), I32)
    sources = [dest, blocks, probe_keys, group_ids, words, section_weights[0]]
    shared, *packed = run(
        functools.partial(pack_first, few, slots),
        [me.reshape(1)] + sources,
        [((columns + micros * block_count, columns), BF16)]
        + ([((height, columns), BF16)] * owners if few else [((owners, height, columns), BF16)]),
        [pltpu.SMEM(dest.shape, I32)]
        + [pltpu.VMEM(source.shape, source.dtype) for source in sources[1:]]
        + [
            pltpu.VMEM((owners, height, columns), BF16),
            pltpu.VMEM((owners, height - span, columns), F32),
            counts,
            pltpu.SemaphoreType.DMA((len(sources),)),
        ],
        scalars=(0,),
        away=True,
    )
    if few:
        for k in far_first(owners):
            packed[k] = lax.ppermute(packed[k], "owner", [(i, i ^ k) for i in range(owners)])
    else:
        packed = [lax.all_to_all(packed[0], "owner", split_axis=0, concat_axis=0, tiled=True)]

    received = [shared]
    for k in range(1, sections):
        received.append(lax.ppermute(shared, "section", [(partner(i, k), i) for i in range(sections)]))
    table = run(
        build_table,
        [build_keys.reshape(-1, 128), build_values],
        ((KEYS_OWN, columns), F32),
        [pltpu.VMEM((build_values.shape[0], 2 * columns), BF16)],
        flops=2 * KEYS_OWN * build_keys.shape[0] * columns,
    )
    weights, kept = run(
        functools.partial(place_bits, sections),
        [scalars] + received + [dest],
        [((sections, columns, columns), BF16), ((owners, 8, rows), F32)],
        [pltpu.VMEM((micros * block_count, rows), F32), counts],
        scalars=(0, 1 + sections),
    )
    kept = lax.all_to_all(kept, "owner", split_axis=0, concat_axis=0, tiled=True)

    def scratch(count, group):
        return [
            pltpu.VMEM((count, slots, rows), I32),
            pltpu.VMEM((group * span, columns), F32),
            pltpu.SMEM((count, slots, rows), I32),
            pltpu.SemaphoreType.DMA,
        ]

    work = 2 * KEYS_OWN * span * columns
    sums_shape = ((groups_all, columns), F32)
    if few:
        order = far_first(owners)
        near = [0, order[-1]]
        soon, middle, final = near + order[: owners // 4], order[owners // 2 : -1], order[owners // 4 : owners // 2]
        joined = run(
            functools.partial(join_only, slots),
            [weights, table] + [packed[k] for k in soon],
            ((len(soon), span, columns), BF16),
            scratch(len(soon), 2),
            flops=len(soon) * work,
        )
        sums = run(
            functools.partial(join_sum, slots, span, middle, soon, False),
            [scalars, kept, weights, table] + [packed[k] for k in middle + soon] + [joined],
            sums_shape,
            scratch(len(middle), 2),
            scalars=(0,),
            flops=len(middle) * work,
        )
        sums = run(
            functools.partial(join_sum, slots, span, final, [], True),
            [scalars, kept, weights, table] + [packed[k] for k in final] + [sums],
            sums_shape,
            scratch(len(final), 2),
            scalars=(0,),
            flops=len(final) * work,
        )
    else:
        sums = run(
            functools.partial(join_all, slots, span),
            [kept, weights, table, packed[0]],
            sums_shape,
            scratch(owners, 1),
            flops=owners * work,
        )
    parts = sums.reshape(sections * owners, GRP_DEV, columns)
    parts = lax.all_to_all(parts, ("section", "owner"), split_axis=0, concat_axis=0, tiled=True)
    return jnp.sum(parts, axis=0)


def solution(mesh):
    placed = (
        P("section", "owner", None),
        P("section", "owner"),
        P("section", "owner"),
        P("section", "owner", None),
        P("section", None, "owner"),
        P("section", None, None),
        P("owner"),
        P("owner", None),
    )
    return jax.shard_map(
        local, mesh=mesh, in_specs=placed, out_specs=P(("section", "owner"), None), check_vma=False
    )
```

```python
import functools
import math

import jax
import jax.numpy as jnp
from jax import lax
from jax.experimental import pallas as pl
from jax.experimental.pallas import tpu as pltpu
from jax.sharding import PartitionSpec as P


CAP = 2
KEYS_OWN = 2048
GRP_DEV = 4
FIELDS = 3
BF16 = jnp.bfloat16
F32 = jnp.float32
I32 = jnp.int32


def run(kernel, ins, outs, scratch=(), scalars=(), flops=0, away=False):
    several = isinstance(outs, list)
    shapes = [jax.ShapeDtypeStruct(shape, dtype) for shape, dtype in (outs if several else [outs])]
    held = shapes + [x for k, x in enumerate(ins) if k not in scalars and not away]
    size = sum(math.prod(x.shape) * x.dtype.itemsize for x in held)
    for entry in scratch:
        size += 2 * math.prod(getattr(entry, "shape", ())) * 4
    place = pl.BlockSpec(memory_space=pltpu.VMEM)
    spaces = [pltpu.SMEM if k in scalars else pltpu.HBM if away else pltpu.VMEM for k in range(len(ins))]
    return pl.pallas_call(
        kernel,
        out_shape=shapes if several else shapes[0],
        in_specs=[pl.BlockSpec(memory_space=space) for space in spaces],
        out_specs=[place] * len(shapes) if several else place,
        scratch_shapes=list(scratch),
        compiler_params=pltpu.CompilerParams(vmem_limit_bytes=60 * 2**20 if away else min(size + 4 * 2**20, 60 * 2**20)),
        cost_estimate=pl.CostEstimate(flops=flops, bytes_accessed=size, transcendentals=0) if flops else None,
    )(*ins)


def walk_blocks(dest_ref, count_ref, owners, visit):
    batches, blocks = dest_ref.shape

    def clear(owner, carry):
        count_ref[owner] = 0
        return carry

    lax.fori_loop(0, owners, clear, 0)
    for micro in range(batches):

        def step(block, carry, micro=micro):
            owner = dest_ref[micro, block]
            slot = count_ref[owner]
            count_ref[owner] = slot + 1
            visit(micro, block, owner, slot)
            return carry

        lax.fori_loop(0, blocks, step, 0, unroll=min(blocks, 8))


def put_block(slots, source, owner_at, slot, out_ref, meta_ref):
    values, keys, groups = source
    rows = values.shape[0]
    out_ref[owner_at, pl.ds(pl.multiple_of(slot * rows, rows), rows), :] = values
    high = ((groups >> 7) * (KEYS_OWN // 128) + (keys >> 7)).astype(F32)
    low = (groups & 127).astype(F32)
    for field, part in enumerate((high, (keys & 127).astype(F32), low)):
        meta_ref[owner_at, pl.ds(field * slots + slot, 1), :] = part


def key_of(high, low):
    return (high.astype(I32) & (KEYS_OWN // 128 - 1)) * 128 + low.astype(I32)


def group_of(high, low):
    return (high.astype(I32) // (KEYS_OWN // 128) * 128).astype(F32) + low


def share_bits(words_ref, weight_ref, shared_ref):
    columns = weight_ref.shape[0]
    shared_ref[:columns, :] = weight_ref[...]
    words = words_ref[...]
    micros, length = words.shape
    parts = jnp.concatenate([words & 255, words >> 8], axis=0).astype(F32).astype(BF16)
    width = min(length, 128)
    spread = lax.broadcasted_iota(I32, (width, width * 16), 1) // 16 == lax.broadcasted_iota(I32, (width, width * 16), 0)
    spread = jnp.where(spread, 1.0, 0.0).astype(BF16)
    place = lax.broadcasted_iota(I32, (micros, width * 16), 1) & 15
    for turn in range(length // width):
        found = jnp.dot(parts[:, turn * width : (turn + 1) * width], spread, preferred_element_type=F32).astype(I32)
        bits = (jnp.where(place < 8, found[:micros], found[micros:]) >> (place & 7)) & 1
        stacked = jnp.concatenate([bits[:, k : k + 128] for k in range(0, width * 16, 128)], axis=0)
        start = columns + turn * stacked.shape[0]
        shared_ref[start : start + stacked.shape[0], :] = stacked.astype(F32).astype(BF16)


def pack_first(few, slots, me_ref, *refs):
    sources, shared_ref, outs, held = refs[:6], refs[6], refs[7:-10], refs[-10:-4]
    buffer_ref, meta_ref, count_ref, sems = refs[-4:]
    dest_ref, values_ref, keys_ref, groups_ref, words_ref, weight_ref = held
    owners = buffer_ref.shape[0]
    blocks = dest_ref.shape[1]
    rows = values_ref.shape[1]
    copies = [pltpu.make_async_copy(source, target, sems.at[k]) for k, (source, target) in enumerate(zip(sources, held))]
    for copy in copies:
        copy.start()
    meta_ref[...] = jnp.zeros_like(meta_ref)
    buffer_ref[...] = jnp.zeros_like(buffer_ref)
    me = me_ref[0]
    copies[4].wait()
    copies[5].wait()
    share_bits(words_ref, weight_ref, shared_ref)
    for copy in copies[:4]:
        copy.wait()

    def visit(micro, block, owner, slot):
        lanes = pl.ds(pl.multiple_of(block * rows, rows), rows)
        source = (values_ref[micro * blocks + block], keys_ref[pl.ds(micro, 1), lanes], groups_ref[pl.ds(micro, 1), lanes])
        put_block(slots, source, owner ^ me if few else owner, slot, buffer_ref, meta_ref)

    walk_blocks(dest_ref, count_ref, owners, visit)
    buffer_ref[:, slots * rows :, :] = meta_ref[...].astype(BF16)
    if few:
        for k, out in enumerate(outs):
            out[...] = buffer_ref[k]
    else:
        outs[0][...] = buffer_ref[...]


def build_table(keys_ref, values_ref, out_ref, wide_ref):
    chunks, lanes = keys_ref.shape
    columns = values_ref.shape[1]
    tiles = out_ref.shape[0] // lanes // 2
    sub = lax.broadcasted_iota(I32, (lanes, lanes), 0)
    keys = keys_ref[...]
    upper = jnp.where(keys >= tiles * lanes, 1.0, 0.0).T
    middle = (keys >> 7) & (tiles - 1)
    low = []
    for chunk in range(chunks):
        low.append(jnp.where(sub == (keys[chunk : chunk + 1] & (lanes - 1)), 1.0, 0.0).astype(BF16))
        flag = jnp.broadcast_to(upper[:, chunk : chunk + 1], (lanes, columns)).astype(BF16)
        part = values_ref[chunk * lanes : (chunk + 1) * lanes, :]
        high_part = part * flag
        wide_ref[chunk * lanes : (chunk + 1) * lanes, :columns] = part - high_part
        wide_ref[chunk * lanes : (chunk + 1) * lanes, columns:] = high_part

    def tile_step(tile, carry):
        here = jnp.where(middle == tile, 1.0, 0.0)
        hot = [low[chunk] * jnp.broadcast_to(here[chunk : chunk + 1], (lanes, lanes)).astype(BF16) for chunk in range(chunks)]
        total = jnp.dot(jnp.concatenate(hot, axis=1), wide_ref[...], preferred_element_type=F32)
        out_ref[pl.ds(pl.multiple_of(tile * lanes, lanes), lanes), :] = total[:, :columns]
        out_ref[pl.ds(pl.multiple_of((tiles + tile) * lanes, lanes), lanes), :] = total[:, columns:]
        return carry

    lax.fori_loop(0, tiles, tile_step, 0)


def place_bits(sections, scalar_ref, *refs):
    shared, (dest_ref, weights_ref, out_ref, kept_ref, count_ref) = refs[:sections], refs[sections:]
    owners = out_ref.shape[0]
    batches, blocks = dest_ref.shape
    columns = weights_ref.shape[1]
    home = scalar_ref[sections + 1]
    kept = shared[0][columns:, :].astype(F32)
    for ref in shared[1:]:
        kept = kept * ref[columns:, :].astype(F32)
    kept_ref[...] = kept
    micros = kept.shape[0] // blocks
    for k, ref in enumerate(shared):
        weights_ref[scalar_ref[k]] = (ref[:columns, :].astype(F32) * 0.5).astype(BF16)
    out_ref[...] = jnp.zeros_like(out_ref)

    def visit(micro, block, owner, slot):
        out_ref[owner, pl.ds(slot, 1), :] = kept_ref[pl.ds(block * micros + home * batches + micro, 1), :]

    walk_blocks(dest_ref, count_ref, owners, visit)


def chain(values, weights):
    for weight in weights:
        half = jnp.dot(values, weight, preferred_element_type=F32)
        values = (values.astype(F32) + (half + half * jnp.tanh(half))).astype(BF16)
    return values


def start_keys(parts, slots, span, keys_ref, places_ref, sem):
    for k, part in enumerate(parts):
        meta = part[span:, :].astype(F32)
        keys_ref[k] = key_of(meta[:slots], meta[slots : 2 * slots])
    copy = pltpu.make_async_copy(keys_ref, places_ref, sem)
    copy.start()
    return copy


def join_parts(parts, first, slots, span, weights, table_ref, found_ref, places_ref, copy=None):
    rows = span // slots
    if copy is not None:
        copy.wait()
    values = chain(jnp.concatenate([part[:span, :] for part in parts], axis=0), weights)
    for block in range(len(parts) * slots):
        for row in range(rows):
            place = places_ref[first + block // slots, block % slots, row]
            found_ref[block * rows + row : block * rows + row + 1, :] = table_ref[pl.ds(place, 1), :]
    return (values.astype(F32) * found_ref[...]).astype(BF16)


def sums_of(parts, kepts, joined, slots, span, groups):
    sub = lax.broadcasted_iota(I32, (groups, span // slots), 0).astype(F32)
    hot = []
    for part, kept in zip(parts, kepts):
        meta = part[span:, :].astype(F32)
        keys = group_of(meta[:slots], meta[2 * slots : 3 * slots])
        keys = jnp.where(kept[:slots] > 0.5, keys, -1.0)
        hot += [jnp.where(sub == keys[j : j + 1], 1.0, 0.0).astype(BF16) for j in range(slots)]
    return jnp.dot(jnp.concatenate(hot, axis=1), joined, preferred_element_type=F32)


def join_only(slots, weights_ref, table_ref, *refs):
    parts, (out_ref, keys_ref, found_ref, places_ref, sem) = refs[:-5], refs[-5:]
    span = out_ref.shape[1]
    group = found_ref.shape[0] // span
    copy = start_keys(parts, slots, span, keys_ref, places_ref, sem)
    weights = [weights_ref[j] for j in range(weights_ref.shape[0])]
    for at in range(0, len(parts), group):
        first = None if at else copy
        joined = join_parts(parts[at : at + group], at, slots, span, weights, table_ref, found_ref, places_ref, first)
        out_ref[at : at + group] = joined.reshape(group, span, joined.shape[1])


def join_sum(slots, span, new, old, scalar_ref, kept_ref, weights_ref, table_ref, *refs):
    news, olds, refs = refs[: len(new)], refs[len(new) : len(new) + len(old)], refs[len(new) + len(old) :]
    joined_ref, out_ref, keys_ref, found_ref, places_ref, sem = refs
    groups = out_ref.shape[0]
    group = found_ref.shape[0] // span
    me = scalar_ref[weights_ref.shape[0]]
    copy = start_keys(news, slots, span, keys_ref, places_ref, sem)
    weights = [weights_ref[j] for j in range(weights_ref.shape[0])]
    joined = joined_ref[...].reshape(len(old) * span, out_ref.shape[1])
    total = sums_of(olds, [kept_ref[me ^ k] for k in old], joined, slots, span, groups)
    for at in range(0, len(new), group):
        these = news[at : at + group]
        first = None if at else copy
        joined = join_parts(these, at, slots, span, weights, table_ref, found_ref, places_ref, first)
        total += sums_of(these, [kept_ref[me ^ k] for k in new[at : at + group]], joined, slots, span, groups)
    out_ref[...] = total


def join_all(slots, span, kept_ref, weights_ref, table_ref, first_ref, out_ref, keys_ref, found_ref, places_ref, sem):
    groups = out_ref.shape[0]
    meta = first_ref[:, span:, :].astype(F32)
    keys_ref[...] = key_of(meta[:, :slots], meta[:, slots : 2 * slots])
    copy = pltpu.make_async_copy(keys_ref, places_ref, sem)
    copy.start()
    weights = [weights_ref[j] for j in range(weights_ref.shape[0])]
    out_ref[...] = jnp.zeros_like(out_ref)
    copy.wait()

    def step(source, carry):
        part = first_ref.at[source]
        joined = join_parts([part], source, slots, span, weights, table_ref, found_ref, places_ref)
        out_ref[...] += sums_of([part], [kept_ref[source]], joined, slots, span, groups)
        return carry

    lax.fori_loop(0, first_ref.shape[0], step, 0)


def few_owners(owners):
    return 4 < owners <= 8 and owners & (owners - 1) == 0


def far_first(owners):
    return sorted(range(1, owners), key=lambda k: -(k // 2) * owners + k)


def local(
    probe_values,
    probe_keys,
    group_ids,
    block_dest,
    filter_bits,
    section_weights,
    build_keys,
    build_values,
):
    sections = lax.axis_size("section")
    owners = lax.axis_size("owner")
    home = lax.axis_index("section").astype(I32)
    batches, block_count = block_dest.shape[:2]
    columns = probe_values.shape[2]
    rows = probe_values.shape[1] // block_count
    groups_all = GRP_DEV * sections * owners
    slots = batches * CAP
    span = slots * rows
    height = span + -(-FIELDS * slots // 8) * 8
    few = few_owners(owners)
    paired = sections & (sections - 1) == 0

    def partner(index, k):
        return index ^ k if paired else (index - k) % sections

    me = lax.axis_index("owner").astype(I32)
    scalars = jnp.stack([lax.rem(partner(home, k) - home + sections, sections) for k in range(sections)] + [me, home])
    dest = block_dest.reshape(batches, block_count)
    blocks = probe_values.reshape(batches * block_count, rows, columns)
    words = filter_bits[0]
    micros = words.shape[0]
    counts = pltpu.SMEM((owners,), I32)
    sources = [dest, blocks, probe_keys, group_ids, words, section_weights[0]]
    shared, *packed = run(
        functools.partial(pack_first, few, slots),
        [me.reshape(1)] + sources,
        [((columns + micros * block_count, columns), BF16)]
        + ([((height, columns), BF16)] * owners if few else [((owners, height, columns), BF16)]),
        [pltpu.SMEM(dest.shape, I32)]
        + [pltpu.VMEM(source.shape, source.dtype) for source in sources[1:]]
        + [
            pltpu.VMEM((owners, height, columns), BF16),
            pltpu.VMEM((owners, height - span, columns), F32),
            counts,
            pltpu.SemaphoreType.DMA((len(sources),)),
        ],
        scalars=(0,),
        away=True,
        flops=40 * blocks.size * columns,
    )
    if few:
        for k in far_first(owners):
            packed[k] = lax.ppermute(packed[k], "owner", [(i, i ^ k) for i in range(owners)])
    else:
        packed = [lax.all_to_all(packed[0], "owner", split_axis=0, concat_axis=0, tiled=True)]

    received = [shared]
    for k in range(1, sections):
        received.append(lax.ppermute(shared, "section", [(partner(i, k), i) for i in range(sections)]))
    table = run(
        build_table,
        [build_keys.reshape(-1, 128), build_values],
        ((KEYS_OWN, columns), F32),
        [pltpu.VMEM((build_values.shape[0], 2 * columns), BF16)],
        flops=2 * KEYS_OWN * build_keys.shape[0] * columns,
    )
    weights, kept = run(
        functools.partial(place_bits, sections),
        [scalars] + received + [dest],
        [((sections, columns, columns), BF16), ((owners, 8, rows), F32)],
        [pltpu.VMEM((micros * block_count, rows), F32), counts],
        scalars=(0, 1 + sections),
    )
    kept = lax.all_to_all(kept, "owner", split_axis=0, concat_axis=0, tiled=True)

    def scratch(count, group):
        return [
            pltpu.VMEM((count, slots, rows), I32),
            pltpu.VMEM((group * span, columns), F32),
            pltpu.SMEM((count, slots, rows), I32),
            pltpu.SemaphoreType.DMA,
        ]

    work = 2 * KEYS_OWN * span * columns
    sums_shape = ((groups_all, columns), F32)
    if few:
        order = far_first(owners)
        soon = [0, order[-1]] + order[: owners // 4]
        rest = order[owners // 2 : -1] + order[owners // 4 : owners // 2]
        joined = run(
            functools.partial(join_only, slots),
            [weights, table] + [packed[k] for k in soon],
            ((len(soon), span, columns), BF16),
            scratch(len(soon), 4),
            flops=len(soon) * work,
        )
        sums = run(
            functools.partial(join_sum, slots, span, rest, soon),
            [scalars, kept, weights, table] + [packed[k] for k in rest + soon] + [joined],
            sums_shape,
            scratch(len(rest), 4),
            scalars=(0,),
            flops=len(rest) * work,
        )
    else:
        sums = run(
            functools.partial(join_all, slots, span),
            [kept, weights, table, packed[0]],
            sums_shape,
            scratch(owners, 1),
            flops=owners * work,
        )
    parts = sums.reshape(sections * owners, GRP_DEV, columns)
    parts = lax.all_to_all(parts, ("section", "owner"), split_axis=0, concat_axis=0, tiled=True)
    return jnp.sum(parts, axis=0)


def solution(mesh):
    placed = (
        P("section", "owner", None),
        P("section", "owner"),
        P("section", "owner"),
        P("section", "owner", None),
        P("section", None, "owner"),
        P("section", None, None),
        P("owner"),
        P("owner", None),
    )
    return jax.shard_map(
        local, mesh=mesh, in_specs=placed, out_specs=P(("section", "owner"), None), check_vma=False
    )
```
